32 devices in a mesh: groups: 2 (over x), tok: 16 (over z, y, core).
Axes of the slice: x: 2, y: 2, z: 4, core: 2. Of those that a mesh axis runs over, the one named last changes fastest.
Arguments:
- activations: bfloat16 [32, 128, 768], P(('groups', 'tok')), parts along dimension 0, may hold values from -32 to 32
- pair_repr: bfloat16 [256, 128, 128], P('groups', 'tok'), parts along dimension 0, may hold values from -6 to 6
- pair_gain: float32 [128], replicated, may hold values from 0.5 to 1.5
- bias_weight: float32 [128, 16], replicated, may hold values from -0.5 to 0.5
- proj_weight: bfloat16 [768, 3072], replicated, may hold values from -0.21875 to 0.21875
- query_bias: float32 [768], replicated, may hold values from -5 to 5
- out_weight: bfloat16 [768, 768], replicated, may hold values from -0.21875 to 0.21875
- token_mask: int32 [256], P('groups'), parts along dimension 0, may hold values 0 or 1
- out_cotangent: bfloat16 [32, 128, 768], P(('groups', 'tok')), parts along dimension 0, may hold values from -6 to 6
Outputs:
- grad_activations: bfloat16 [32, 128, 768], P(('groups', 'tok')), parts along dimension 0
- grad_pair: bfloat16 [256, 128, 128], P('groups', 'tok'), parts along dimension 0
- grad_proj: float32 [1536, 3072], P(('groups', 'tok')), parts along dimension 0
- grad_out_weight: float32 [1536, 768], P(('groups', 'tok')), parts along dimension 0
- grad_query_bias: float32 [1536], P('groups'), parts along dimension 0
- grad_bias_weight: float32 [256, 16], P('groups'), parts along dimension 0
- grad_pair_gain: float32 [256], P('groups'), parts along dimension 0
The draws below stay inside these ranges and needn't reach their ends.
There are 2 independent parts, one for each index of `groups`. The reference program is written for one: setup_inputs(seed, part) draws one part's arguments, and reference() takes and returns one part's arrays. A program takes and returns all parts, laid end to end along the dimension named above; an argument that names none is the same for every part. Nothing has to cross between parts.
All inputs are finite; a program needn't handle non-finite values.
Results may differ from the reference program's by a relative error of at most 0.015.
The reference program's roundings to bfloat16 on the way count: a program that leaves them out, or rounds other values in their place, can miss the bound.
Values may be sent and summed in bfloat16 or wider, within the bound.
A program may use at most 128 MiB of HBM per device.

```python
import jax
import jax.numpy as jnp
from jax import lax

D = 768
HEADS = 16
HD = 48
CZ = 128
NTOK = 128
SAMPLES = 16


def draw_activations(key, part):
    values = jax.random.truncated_normal(key, -4.0, 4.0, (SAMPLES, NTOK, D), jnp.float32)
    return values.astype(jnp.bfloat16)


def set_ends(result, stream_key, least, top_value):
    spot = [jax.random.randint(jax.random.fold_in(stream_key, axis), (), 0, length) for axis, length in enumerate(result.shape)]
    main_axis = result.shape.index(max(result.shape))
    next_to = spot[:main_axis] + [(spot[main_axis] + 1) % result.shape[main_axis]] + spot[main_axis + 1:]
    return result.at[tuple(spot)].set(least).at[tuple(next_to)].set(top_value)


def with_spikes(drawn, rng, source, target, blocks, factor):
    def block_of(axis_at):
        return (jnp.arange(drawn.shape[axis_at]) // (drawn.shape[axis_at] // blocks)).reshape((-1,) + (1,) * (drawn.ndim - 1 - axis_at))

    one_side = jax.random.permutation(rng, blocks)[block_of(target)]
    other_side = (block_of(target) + blocks // 2) % blocks
    return jnp.where((block_of(source) == one_side) | (block_of(source) == other_side), factor * drawn, drawn)


def shard_levels(rng, shape, shards, smallest, top_value):
    loudness = 1.0
    for dim, shards_of in shards:
        draws = jax.random.uniform(jax.random.fold_in(jax.random.fold_in(rng, 6), dim), (shards_of,), jnp.float32, smallest / len(shards), top_value / len(shards))
        loudness = loudness * jnp.repeat(jnp.exp(draws), shape[dim] // shards_of).reshape((-1,) + (1,) * (len(shape) - 1 - dim))
    return loudness


def scatter_about(rng, dims, scale, reach, shards=(), dtype=jnp.bfloat16):
    values = jax.random.normal(rng, dims, jnp.float32) * scale
    if len(shards) > 0:
        values = shard_levels(rng, dims, shards, -0.22, 0.18) * values
    return jnp.clip(values, min=-reach, max=reach).astype(dtype)


def gaussian_with(key, dims, scale, reach, cuts, heavy, kind=jnp.bfloat16):
    drawn = scale * jax.random.normal(key, dims, jnp.float32)
    if cuts:
        drawn = drawn * shard_levels(key, dims, cuts, -0.22, 0.18)
    return jnp.clip(with_spikes(drawn, jax.random.fold_in(key, 3), *heavy), -reach, reach).astype(kind)


def setup_inputs(seed: int = 0, part: int = 0) -> dict:
    seeds = jax.random.split(jax.random.key(seed), 10)
    own_keys = jax.random.split(jax.random.fold_in(seeds[9], part), 10)
    return {
        "activations": draw_activations(jax.random.fold_in(jax.random.fold_in(seeds[9], part), 71), part),
        "pair_repr": scatter_about(own_keys[1], (NTOK, NTOK, CZ), 1.0, 6.0, ((1, 16),)),
        "pair_gain": jnp.clip(1.0 + 0.1 * jax.random.normal(seeds[2], (CZ,), jnp.float32), 0.5, 1.5),
        "bias_weight": scatter_about(seeds[3], (CZ, HEADS), CZ ** -0.5, 0.5, (), jnp.float32),
        "proj_weight": scatter_about(seeds[4], (D, 4 * D), D ** -0.5, 0.21875),
        "query_bias": scatter_about(seeds[5], (D,), 1.0, 5.0, (), jnp.float32),
        "out_weight": scatter_about(seeds[6], (D, D), D ** -0.5, 0.21875),
        "token_mask": set_ends((jax.random.randint(own_keys[7], (NTOK,), 0, 8) < 7).astype(jnp.int32), jax.random.fold_in(own_keys[7], 1), 0, 1),
        "out_cotangent": gaussian_with(own_keys[8], (SAMPLES, NTOK, D), 1.0, 6.0, ((0, 16),), (0, 2, 16, 2.0)),
    }


EPSILON = 1e-05
MASK_PENALTY = 10000.0

def reference(activations, pair_repr, pair_gain, bias_weight, proj_weight, query_bias, out_weight, token_mask, out_cotangent):
    feature = activations.shape[2]
    all_tokens = activations.shape[1]
    softmax_scale = HD ** (-0.5)
    act_rows = activations.reshape(SAMPLES * all_tokens, feature)
    cot_rows = out_cotangent.reshape(SAMPLES * all_tokens, feature)
    proj = jnp.dot(act_rows, proj_weight, preferred_element_type=jnp.float32)
    shift = jnp.concatenate([query_bias, jnp.zeros((2 * feature,), jnp.float32)])
    qkv_rows = (proj[:, :3 * feature] + shift[None, :]).astype(jnp.bfloat16)
    gate = jax.nn.sigmoid(proj[:, 3 * feature:]).astype(jnp.bfloat16)
    pair_f = pair_repr.astype(jnp.float32)
    mean_z = lax.optimization_barrier(jnp.mean(pair_f, axis=-1, keepdims=True))
    centred = pair_f - mean_z
    rstd = lax.rsqrt(lax.optimization_barrier(jnp.mean(centred * centred, axis=-1, keepdims=True)) + EPSILON)
    normed = centred * rstd
    scaled = normed * pair_gain
    pair_bias = jnp.einsum('ijc,ch->hij', scaled, bias_weight, precision=lax.Precision.HIGHEST).astype(jnp.bfloat16)
    bias_full = pair_bias.astype(jnp.float32)
    key_bias = (token_mask.astype(jnp.float32) - 1.0) * MASK_PENALTY
    grad_gated = jnp.dot(cot_rows, out_weight.T, preferred_element_type=jnp.float32).astype(jnp.bfloat16)
    qkv_s = qkv_rows.reshape(SAMPLES, all_tokens, 3, HEADS, HD)
    gate_s = gate.reshape(SAMPLES, all_tokens, feature)
    grad_s_in = grad_gated.reshape(SAMPLES, all_tokens, feature)

    def per_sample(total, pieces):
        qkv, gate_one, grad_one = pieces
        query = qkv[:, 0].transpose(1, 0, 2).astype(jnp.float32)
        keys = qkv[:, 1].transpose(1, 0, 2).astype(jnp.float32)
        values = qkv[:, 2].transpose(1, 0, 2).astype(jnp.float32)
        scores = jnp.einsum('hid,hjd->hij', query, keys) * softmax_scale + bias_full + key_bias[None, None, :]
        peak = lax.optimization_barrier(jnp.max(scores, axis=-1, keepdims=True))
        expo = jnp.exp(scores - peak)
        probs = expo / lax.optimization_barrier(jnp.sum(expo, axis=-1, keepdims=True))
        probs_b = probs.astype(jnp.bfloat16).astype(jnp.float32)
        attended = jnp.einsum('hij,hjd->hid', probs_b, values).astype(jnp.bfloat16)
        attended = attended.transpose(1, 0, 2).reshape(all_tokens, feature).astype(jnp.float32)
        gate32 = gate_one.astype(jnp.float32)
        grad32 = grad_one.astype(jnp.float32)
        gated = (gate32 * attended).astype(jnp.bfloat16)
        grad_att = (grad32 * gate32).astype(jnp.bfloat16)
        grad_logit = (grad32 * attended * gate32 * (1.0 - gate32)).astype(jnp.bfloat16)
        grad_heads = grad_att.reshape(all_tokens, HEADS, HD).transpose(1, 0, 2).astype(jnp.float32)
        grad_probs = jnp.einsum('hid,hjd->hij', grad_heads, values)
        grad_scores = probs * (grad_probs - lax.optimization_barrier(jnp.sum(probs * grad_probs, axis=-1, keepdims=True)))
        scores_b = grad_scores.astype(jnp.bfloat16).astype(jnp.float32)
        grad_query = jnp.einsum('hij,hjd->hid', scores_b, keys) * softmax_scale
        grad_value = jnp.einsum('hij,hid->hjd', probs_b, grad_heads)
        grad_key = jnp.einsum('hij,hid->hjd', scores_b, query) * softmax_scale
        stacked = jnp.stack([grad_query, grad_key, grad_value], axis=0).astype(jnp.bfloat16)
        stacked = stacked.transpose(2, 0, 1, 3).reshape(all_tokens, 3 * feature)
        rows_out = jnp.concatenate([stacked, grad_logit], axis=1)
        return (total + grad_scores, (rows_out, gated))
    start_total = jnp.zeros((HEADS, all_tokens, all_tokens), jnp.float32)
    grad_bias, outs = lax.scan(per_sample, start_total, (qkv_s, gate_s, grad_s_in))
    grad_rows = outs[0].reshape(SAMPLES * all_tokens, 4 * feature)
    gated_rows = outs[1].reshape(SAMPLES * all_tokens, feature)
    grad_proj = jnp.dot(act_rows.T, grad_rows, preferred_element_type=jnp.float32)
    grad_out_weight = jnp.dot(gated_rows.T, cot_rows, preferred_element_type=jnp.float32)
    grad_query_bias = lax.optimization_barrier(jnp.sum(grad_rows[:, :feature].astype(jnp.float32), axis=0))
    grad_activations = jnp.dot(grad_rows, proj_weight.T, preferred_element_type=jnp.float32).astype(jnp.bfloat16)
    grad_zg = jnp.einsum('hij,ch->ijc', grad_bias, bias_weight, precision=lax.Precision.HIGHEST)
    grad_bias_weight = jnp.einsum('ijc,hij->ch', scaled, grad_bias, precision=lax.Precision.HIGHEST)
    grad_pair_gain = lax.optimization_barrier(jnp.sum(normed * grad_zg, axis=(0, 1)))
    grad_norm = grad_zg * pair_gain
    grad_pair = (grad_norm - lax.optimization_barrier(jnp.mean(grad_norm, axis=-1, keepdims=True)) - normed * lax.optimization_barrier(jnp.mean(grad_norm * normed, axis=-1, keepdims=True))) * rstd
    return (grad_activations.reshape(SAMPLES, all_tokens, feature), grad_pair.astype(jnp.bfloat16), grad_proj, grad_out_weight, grad_query_bias, grad_bias_weight, grad_pair_gain)
```

```python
import functools

import jax
import jax.numpy as jnp
from jax import lax
from jax.experimental import pallas as pl
from jax.experimental.pallas import tpu as pltpu
from jax.sharding import PartitionSpec as P

HEADS = 16
HD = 48
EPSILON = 1e-05
MASK_PENALTY = 10000.0
F32 = jnp.float32
BF16 = jnp.bfloat16
INNER = 4


def exchange_kernel(kinds, tok, *refs):
    count = len(kinds)
    ins, outs = refs[:count], refs[count : 2 * count]
    sends, recvs, local_sem = refs[2 * count : 3 * count], refs[3 * count : 4 * count], refs[4 * count]
    me = lax.axis_index("tok")
    group = me // INNER
    place = me % INNER
    across = place + 1 - 2 * (place % 2)
    beside = place + 2 - 4 * (place // 2)
    barrier = pltpu.get_barrier_semaphore()
    for step in range(1, tok):
        pl.semaphore_signal(barrier, inc=1, device_id={"tok": (me + step) % tok})
    pl.semaphore_wait(barrier, tok - 1)

    def send(k, slot, src, dst, peer):
        copy = pltpu.make_async_remote_copy(
            src_ref=src,
            dst_ref=dst,
            send_sem=sends[k].at[slot],
            recv_sem=recvs[k].at[slot],
            device_id={"tok": peer},
        )
        copy.start()
        return copy

    pending, relays, local = [], [], []
    for k, kind in enumerate(kinds):
        x, out = ins[k], outs[k]
        if kind == "near":
            first = send(k, 0, x, out.at[place], group * INNER + beside)
            pending.append(send(k, 1, x, out.at[place], group * INNER + across))
            relays.append((k, first, out.at[beside]))
        elif kind in ("all", "each"):
            for step in range(1, tok):
                peer = (me + step) % tok
                pending.append(send(k, step - 1, x if kind == "all" else x.at[peer], out.at[me], peer))
        elif kind == "near_each":
            for step in range(1, INNER):
                other = (place + step) % INNER
                pending.append(send(k, step - 1, x.at[other], out.at[place], group * INNER + other))
        else:
            for step in range(1, tok // INNER):
                other = (group + step) % (tok // INNER)
                pending.append(send(k, step - 1, x.at[other], out.at[group], other * INNER + place))
    for k, kind in enumerate(kinds):
        mine = {"all": me, "each": me, "near": place, "near_each": place, "far_each": group}[kind]
        own = ins[k] if kind in ("all", "near") else ins[k].at[mine]
        copy = pltpu.make_async_copy(own, outs[k].at[mine], local_sem.at[k])
        copy.start()
        local.append(copy)
    for k, first, block in relays:
        first.wait()
        pending.append(send(k, 2, block, block, group * INNER + across))
    for copy in local + pending:
        copy.wait()


def exchange(arrays, kinds, tok, collective_id):
    sizes = {"all": tok, "each": tok, "near": INNER, "near_each": INNER, "far_each": tok // INNER}
    shapes = []
    for x, kind in zip(arrays, kinds):
        block = x.shape if kind in ("all", "near") else x.shape[1:]
        shapes.append(jax.ShapeDtypeStruct((sizes[kind],) + block, x.dtype))
    sems = [pltpu.SemaphoreType.DMA((max(3, sizes[kind] - 1),)) for kind in kinds]
    return pl.pallas_call(
        functools.partial(exchange_kernel, kinds, tok),
        out_shape=shapes,
        in_specs=[pl.BlockSpec(memory_space=pltpu.VMEM)] * len(kinds),
        out_specs=[pl.BlockSpec(memory_space=pltpu.VMEM)] * len(kinds),
        scratch_shapes=sems + sems + [pltpu.SemaphoreType.DMA((len(kinds),))],
        compiler_params=pltpu.CompilerParams(
            collective_id=collective_id, has_side_effects=True, vmem_limit_bytes=40 * 2**20
        ),
        name=f"exchange_{collective_id}",
    )(*arrays)


def attention(query, keys, values, gate, grad_gated, bias_t, key_bias):
    scale = HD ** (-0.5)
    scores = jnp.einsum("hdj,hdi->hji", keys, query, preferred_element_type=F32) * scale
    scores = scores + bias_t.transpose(1, 0, 2).astype(F32) + key_bias[None, :, None]
    peak = jnp.max(scores, axis=1, keepdims=True)
    expo = jnp.exp(scores - peak)
    probs = expo / jnp.sum(expo, axis=1, keepdims=True)
    probs_b = probs.astype(BF16)
    attended = jnp.einsum("hdj,hji->hdi", values, probs_b, preferred_element_type=F32).astype(BF16)
    gate32 = gate.astype(F32)
    grad32 = grad_gated.astype(F32)
    att32 = attended.astype(F32)
    gated = (gate32 * att32).astype(BF16)
    grad_att = (grad32 * gate32).astype(BF16)
    grad_logit = (grad32 * att32 * gate32 * (1.0 - gate32)).astype(BF16)
    grad_probs = jnp.einsum("hdj,hdi->hji", values, grad_att, preferred_element_type=F32)
    grad_scores = probs * (grad_probs - jnp.sum(probs * grad_probs, axis=1, keepdims=True))
    scores_b = grad_scores.astype(BF16)
    grad_query = (jnp.einsum("hdj,hji->hdi", keys, scores_b, preferred_element_type=F32) * scale).astype(BF16)
    grad_key = (jnp.einsum("hdi,hji->hdj", query, scores_b, preferred_element_type=F32) * scale).astype(BF16)
    grad_value = jnp.einsum("hdi,hji->hdj", grad_att, probs_b, preferred_element_type=F32).astype(BF16)
    return jnp.stack([grad_query, grad_key, grad_value, grad_logit]), gated, grad_scores


def general_plan(activations, pair_repr, pair_gain, bias_weight, proj_weight, query_bias, out_weight, token_mask, out_cotangent):
    samples, tokens, feature = activations.shape
    tok = lax.axis_size("tok")
    cols = pair_repr.shape[1]
    act = activations.reshape(samples * tokens, feature)
    cot = out_cotangent.reshape(samples * tokens, feature)
    pair_f = pair_repr.astype(F32)
    centred = pair_f - jnp.mean(pair_f, axis=-1, keepdims=True)
    rstd = lax.rsqrt(jnp.mean(centred * centred, axis=-1, keepdims=True) + EPSILON)
    normed = centred * rstd
    scaled = normed * pair_gain
    bias_cols = jnp.einsum("ijc,ch->jhi", scaled, bias_weight, precision=lax.Precision.HIGHEST).astype(BF16)
    outer = tok // INNER
    shard = feature // tok

    def near_blocks(x):
        blocks = x.reshape(outer, INNER, shard, samples * tokens).transpose(1, 0, 2, 3)
        return blocks.reshape(INNER, outer * shard, samples * tokens)

    bias_t, cot_near, act_near = exchange(
        (bias_cols, cot, near_blocks(act.T)), ("all", "near", "near_each"), tok, 0
    )
    bias_t = bias_t.reshape((tok * cols,) + bias_cols.shape[1:])
    proj = jnp.einsum("tf,fn->nt", act, proj_weight, preferred_element_type=F32)
    proj = proj.reshape(4, feature, samples * tokens)
    query = (proj[0] + query_bias[:, None]).astype(BF16)
    keys = proj[1].astype(BF16)
    values = proj[2].astype(BF16)
    gate = jax.nn.sigmoid(proj[3]).astype(BF16)
    grad_gated = jnp.einsum("tn,mn->mt", cot, out_weight, preferred_element_type=F32).astype(BF16)
    key_bias = (token_mask.astype(F32) - 1.0) * MASK_PENALTY

    def heads_of(x):
        return x.reshape(HEADS, HD, samples, tokens).transpose(2, 0, 1, 3)

    grads, gated, grad_scores = jax.vmap(attention, in_axes=(0, 0, 0, 0, 0, None, None))(
        heads_of(query), heads_of(keys), heads_of(values), heads_of(gate), heads_of(grad_gated), bias_t, key_bias
    )
    grad_rows = grads.transpose(1, 2, 3, 0, 4).reshape(4 * feature, samples * tokens)
    gated_t = gated.transpose(1, 2, 0, 3).reshape(feature, samples * tokens)
    score_sum = jnp.sum(grad_scores, axis=0).astype(BF16)
    outgoing = score_sum.reshape(HEADS, tok, cols, tokens).transpose(1, 2, 0, 3)
    received, rows_near, gated_near = exchange(
        (outgoing, grad_rows, near_blocks(gated_t)), ("each", "near", "near_each"), tok, 1
    )
    grad_bias = jnp.sum(received.astype(F32), axis=0)
    grad_activations = jnp.einsum("nt,fn->tf", grad_rows, proj_weight, preferred_element_type=F32).astype(BF16)
    grad_zg = jnp.einsum("jhi,ch->ijc", grad_bias, bias_weight, precision=lax.Precision.HIGHEST)
    weight_part = jnp.einsum("ijc,jhi->ch", scaled, grad_bias, precision=lax.Precision.HIGHEST)
    gain_part = jnp.sum(normed * grad_zg, axis=(0, 1))
    query_part = jnp.sum(grad_rows[:feature].astype(F32), axis=1)
    small = jnp.concatenate([query_part, weight_part.reshape(-1), gain_part])
    small = jnp.pad(small, (0, -small.size % 1024)).reshape(-1, 128)
    first = jnp.einsum("srt,snt->rn", act_near, rows_near, preferred_element_type=F32)
    second = jnp.einsum("srt,stn->rn", gated_near, cot_near, preferred_element_type=F32)
    terms = jnp.concatenate([first.astype(BF16), second.astype(BF16)], axis=1)
    terms, small = exchange((terms.reshape(outer, shard, -1), small), ("far_each", "all"), tok, 2)
    weight_grads = jnp.sum(terms.astype(F32), axis=0)
    small = jnp.sum(small, axis=0).reshape(-1)
    grad_norm = grad_zg * pair_gain
    grad_pair = (
        grad_norm
        - jnp.mean(grad_norm, axis=-1, keepdims=True)
        - normed * jnp.mean(grad_norm * normed, axis=-1, keepdims=True)
    ) * rstd
    split = feature + weight_part.size
    return (
        grad_activations.reshape(samples, tokens, feature),
        grad_pair.astype(BF16),
        weight_grads[:, : 4 * feature],
        weight_grads[:, 4 * feature :],
        small[:feature],
        small[feature:split].reshape(weight_part.shape),
        small[split : split + pair_gain.shape[0]],
    )


NN = (((1,), (0,)), ((), ()))
NT = (((1,), (1,)), ((), ()))
TN = (((0,), (0,)), ((), ()))


def dot(a, b, dims, precision=None):
    return lax.dot_general(a, b, dims, precision=precision, preferred_element_type=F32)


def fused_kernel(
    tok,
    act,
    cot,
    pair,
    gain,
    bias_w,
    query_bias,
    mask,
    proj_hbm,
    out_w_hbm,
    grad_act,
    grad_pair,
    grad_w,
    grad_out,
    small_out,
    proj_w,
    out_w,
    proj_t,
    act_all,
    cot_all,
    act_t,
    query_col,
    normed,
    rstd,
    bias_f,
    bias_send,
    bias_recv,
    q_s,
    k_s,
    v_s,
    g_s,
    gg_s,
    ga_s,
    gated_s,
    probs_s,
    rows_a,
    rows_b,
    rows_back,
    term_send,
    term_recv,
    wout_send,
    wout_recv,
    score_send,
    score_recv,
    score_f,
    small_a,
    small_b,
    recv_a,
    recv_b,
    local_sem,
    act_sems,
    bias_sems,
    term_sems,
    wout_sems,
    back_sems,
    score_sems,
    small_sems,
):
    tokens, feature = act.shape
    inner = INNER
    planes = tok // inner
    group_heads, head_dim = q_s.shape[0], q_s.shape[1]
    cols = pair.shape[0]
    channels = pair.shape[2]
    span = group_heads * head_dim
    window = proj_t.shape[1]
    shard = feature // tok
    scale = head_dim ** (-0.5)
    me = lax.axis_index("tok")
    plane = me // inner
    place = me % inner
    across = place + 1 - 2 * (place % 2)
    beside = place + 2 - 4 * (place // 2)
    diagonal = across + 2 - 4 * (across // 2)
    base = pl.multiple_of((place * span) // 128 * 128, 128)
    offset = pl.multiple_of(place * span - (place * span) // 128 * 128, 64)

    load_proj = pltpu.make_async_copy(proj_hbm, proj_w, local_sem.at[0])
    load_proj.start()
    load_out = pltpu.make_async_copy(
        out_w_hbm.at[pl.ds(pl.multiple_of(place * span, 64), span)], out_w, local_sem.at[1]
    )
    load_out.start()

    barrier = pltpu.get_barrier_semaphore()
    for step in range(1, tok):
        pl.semaphore_signal(barrier, inc=1, device_id={"tok": (me + step) % tok})
    pl.semaphore_wait(barrier, tok - 1)

    def remote(src, dst, sems, slot, peer, arrival=None):
        return pltpu.make_async_remote_copy(
            src_ref=src,
            dst_ref=dst,
            send_sem=sems.at[0, slot],
            recv_sem=sems.at[1, slot if arrival is None else arrival],
            device_id={"tok": peer},
        )

    def near(where):
        return plane * inner + where

    sent = []
    act_beside = remote(act, act_all.at[place], act_sems, 0, near(beside))
    act_across = remote(act, act_all.at[place], act_sems, 1, near(across))
    cot_beside = remote(cot, cot_all.at[place], act_sems, 2, near(beside))
    cot_across = remote(cot, cot_all.at[place], act_sems, 3, near(across))
    for copy in (act_beside, act_across, cot_beside, cot_across):
        copy.start()
        sent.append(copy)
    act_all[place] = act[...]
    cot_all[place] = cot[...]

    for j in range(cols):
        x = pair[j].astype(F32)
        centred = x - jnp.mean(x, axis=-1, keepdims=True)
        r = lax.rsqrt(jnp.mean(centred * centred, axis=-1, keepdims=True) + EPSILON)
        y = centred * r
        normed[j] = y
        rstd[j] = r
        part = dot(bias_w[...], y * gain[...], NT, lax.Precision.HIGHEST)
        bias_f[pl.ds(j * HEADS, HEADS), :] = part
    for h in range(HEADS):
        bias_send[h // group_heads, h % group_heads] = bias_f[pl.ds(h, cols, stride=HEADS), :].astype(BF16)
    bias_copies = []
    for step in range(1, tok):
        peer = (me + step) % tok
        copy = remote(bias_send.at[peer % inner], bias_recv.at[me], bias_sems, step - 1, peer)
        copy.start()
        bias_copies.append(copy)
    sent += bias_copies
    bias_recv[me] = bias_send[place]

    row = jnp.broadcast_to(query_bias[:, pl.ds(base, window)], (128, window))
    query_col[...] = row.T
    load_proj.wait()
    for b in range(4):
        proj_t[b] = proj_w[:, pl.ds(pl.multiple_of(feature * b + base, 128), window)].T

    act_beside.wait_recv()
    act_relay = remote(act_all.at[beside], act_all.at[beside], act_sems, 4, near(across))
    act_relay.start()
    cot_beside.wait_recv()
    cot_relay = remote(cot_all.at[beside], cot_all.at[beside], act_sems, 5, near(across))
    cot_relay.start()
    sent += [act_relay, cot_relay]
    act_across.wait_recv()
    act_relay.wait_recv()
    total = inner * tokens
    acts = act_all[...].reshape(total, feature)
    stored = (group_heads, head_dim, total)
    for b, target in enumerate((q_s, k_s, v_s, g_s)):
        block = dot(proj_t[b, pl.ds(offset, span), :], acts, NT)
        if b == 0:
            shift = query_col[pl.ds(offset, span), :]
            block = block + jnp.concatenate([shift] * (total // 128), axis=1)
        if b == 3:
            block = jax.nn.sigmoid(block)
        target[...] = block.astype(BF16).reshape(stored)
    for i in range(inner):
        act_t[:, i * tokens : (i + 1) * tokens] = act_all[i].T
    cot_across.wait_recv()
    cot_relay.wait_recv()
    load_out.wait()
    cots = cot_all[...].reshape(total, feature)
    gg_s[...] = dot(out_w[...], cots, NT).astype(BF16).reshape(stored)
    for copy in bias_copies:
        copy.wait_recv()

    key_row = jnp.broadcast_to((mask[...].astype(F32) - 1.0) * MASK_PENALTY, (tokens, tokens))
    key_bias = key_row.T

    def forward(k, carry):
        bias = bias_recv[:, k].astype(F32).reshape(tokens, tokens)
        for s in range(inner):
            at = slice(s * tokens, (s + 1) * tokens)
            query, keys, values = q_s[k, :, at], k_s[k, :, at], v_s[k, :, at]
            scores = dot(keys, query, TN) * scale + bias + key_bias
            expo = jnp.exp(scores - jnp.max(scores, axis=0, keepdims=True))
            probs = expo / jnp.sum(expo, axis=0, keepdims=True)
            probs_b = probs.astype(BF16)
            attended = dot(values, probs_b, NN).astype(BF16).astype(F32)
            gate32 = g_s[k, :, at].astype(F32)
            grad32 = gg_s[k, :, at].astype(F32)
            grad_att = (grad32 * gate32).astype(BF16)
            gated_s[k, :, at] = (gate32 * attended).astype(BF16)
            ga_s[k, :, at] = grad_att
            rows_a[1, s, k] = (grad32 * attended * gate32 * (1.0 - gate32)).astype(BF16)
            rows_a[0, s, k] = dot(grad_att, probs_b, NT).astype(BF16)
            probs_s[k, s] = probs
        return carry

    lax.fori_loop(0, group_heads, forward, 0)

    order = [planes // 2] + [o for o in range(1, planes) if o != planes // 2] + [0]

    def send_terms(which, rows):
        for o in order:
            target = (plane + o) % planes
            lhs = act_t[pl.ds(pl.multiple_of(target * (inner * shard), 16), inner * shard), :]
            part = dot(lhs, rows, NT)
            term_send[which, target] = part.astype(BF16).reshape(inner, shard, 2 * span)
            for d in range(inner):
                if o == 0 and d == 0:
                    continue
                where = (place + d) % inner
                copy = remote(
                    term_send.at[which, target, where],
                    term_recv.at[which, me],
                    term_sems,
                    which * tok + o * inner + d,
                    target * inner + where,
                )
                copy.start()
                sent.append(copy)
                terms.append(copy)
        term_recv[which, me] = term_send[which, plane, place]

    def send_rows(which, rows):
        for d in range(1, inner):
            where = (place + d) % inner
            copy = remote(
                rows.at[:, where],
                rows_back.at[pl.ds(2 - 2 * which, 2), place],
                back_sems,
                which * inner + d,
                near(where),
            )
            copy.start()
            sent.append(copy)
            backs.append(copy)
        rows_back[pl.ds(2 - 2 * which, 2), place] = rows[:, place]

    def side_by_side(rows):
        return jnp.concatenate([rows[:, s].reshape(2 * span, tokens) for s in range(inner)], axis=1)

    terms, backs = [], []
    send_terms(0, side_by_side(rows_a))
    wout_send[...] = dot(gated_s[...].reshape(span, total), cots, NN).astype(BF16).reshape(wout_send.shape)
    wouts = []
    for d in range(inner):
        where = (place + d) % inner
        copy = remote(wout_send.at[where], wout_recv.at[plane], wout_sems, d, place * inner + where, plane)
        if d == 0:
            @pl.when(place != plane)
            def _():
                copy.start()

            @pl.when(place == plane)
            def _():
                wout_recv[plane] = wout_send[place]
        else:
            copy.start()
        wouts.append(copy)
    send_rows(0, rows_a)

    def backward(k, carry):
        summed = jnp.zeros((tokens, tokens), F32)
        for s in range(inner):
            at = slice(s * tokens, (s + 1) * tokens)
            query, keys, values = q_s[k, :, at], k_s[k, :, at], v_s[k, :, at]
            probs = probs_s[k, s]
            grad_probs = dot(values, ga_s[k, :, at], TN)
            grad_scores = probs * (grad_probs - jnp.sum(probs * grad_probs, axis=0, keepdims=True))
            scores_b = grad_scores.astype(BF16)
            rows_b[0, s, k] = (dot(keys, scores_b, NN) * scale).astype(BF16)
            rows_b[1, s, k] = (dot(query, scores_b, NT) * scale).astype(BF16)
            summed = summed + grad_scores
        score_send[:, k] = summed.reshape(tok, cols, tokens).astype(BF16)
        return carry

    lax.fori_loop(0, group_heads, backward, 0)

    scores = []
    for step in range(1, tok):
        peer = (me + step) % tok
        copy = remote(score_send.at[peer], score_recv.at[me], score_sems, step - 1, peer)
        copy.start()
        scores.append(copy)
    sent += scores
    score_recv[me] = score_send[me]
    send_rows(1, rows_b)
    rows = side_by_side(rows_b)
    send_terms(1, rows)
    query_part = dot(jnp.ones((8, total), BF16), rows[:window], NT)

    for copy in scores:
        copy.wait_recv()
    for q in range(inner):
        for k in range(group_heads):
            part = score_recv[q, k].astype(F32)
            for i in range(1, planes):
                part = part + score_recv[i * inner + q, k].astype(F32)
            h = q * group_heads + k
            score_f[pl.ds(h * cols, cols), :] = part
    weight_part = jnp.zeros((HEADS, channels), F32)
    gain_part = jnp.zeros((8, channels), F32)
    for j in range(cols):
        grad_bias = score_f[pl.ds(j, HEADS, stride=cols), :]
        y = normed[j]
        weight_part = weight_part + dot(grad_bias, y * gain[...], NN, lax.Precision.HIGHEST)
        grad_zg = dot(grad_bias, bias_w[...], TN, lax.Precision.HIGHEST)
        gain_part = gain_part + jnp.sum((y * grad_zg).reshape(tokens // 8, 8, channels), axis=0)
        g = grad_zg * gain[...]
        first = jnp.mean(g, axis=-1, keepdims=True)
        second = jnp.mean(g * y, axis=-1, keepdims=True)
        grad_pair[j] = ((g - first - y * second) * rstd[j]).astype(BF16)
    small_a[0:HEADS, :] = weight_part
    small_a[HEADS : HEADS + 8, :] = gain_part
    small_a[HEADS + 8 : HEADS + 16, :] = query_part[:, :128]
    small_a[HEADS + 16 : HEADS + 24, :] = query_part[:, 128:]
    firsts = []
    for d in range(1, inner):
        where = (place + d) % inner
        copy = remote(small_a, recv_a.at[place], small_sems, d, near(where))
        copy.start()
        firsts.append(copy)
    sent += firsts
    recv_a[place] = small_a[...]
    for copy in firsts:
        copy.wait_recv()
    held = recv_a[0, 0 : HEADS + 8, :]
    for q in range(1, inner):
        held = held + recv_a[q, 0 : HEADS + 8, :]
    small_b[0 : HEADS + 8, :] = held
    for q in range(inner):
        for half in range(2):
            at = HEADS + 8 + 8 * half
            small_b[HEADS + 8 + 2 * q + half : HEADS + 9 + 2 * q + half, :] = recv_a[q, at : at + 1, :]
    seconds = []
    for o in range(1, planes):
        target = (plane + o) % planes
        copy = remote(small_b, recv_b.at[plane], small_sems, inner + o, target * inner + place)
        copy.start()
        seconds.append(copy)
    sent += seconds
    recv_b[plane] = small_b[...]

    for copy in backs:
        copy.wait_recv()
    back = rows_back[...].reshape(4 * feature, tokens)
    for c in range(feature // 128):
        part = dot(proj_w[c * 128 : (c + 1) * 128, :], back, NN)
        grad_act[:, c * 128 : (c + 1) * 128] = part.T.astype(BF16)

    for copy in seconds:
        copy.wait_recv()
    held = recv_b[0]
    for i in range(1, planes):
        held = held + recv_b[i]
    small_out[...] = held

    for d, copy in enumerate(wouts):
        if d == 0:
            @pl.when(place != plane)
            def _():
                copy.wait_send()
        else:
            copy.wait_send()
    for o in range(planes):
        source = (plane + o) % planes
        copy = remote(wout_send.at[0], wout_recv.at[source], wout_sems, 0, near(across), source)
        if o == 0:
            @pl.when(place != plane)
            def _():
                copy.wait_recv()
        else:
            copy.wait_recv()

    held = wout_recv[0].astype(F32)
    for i in range(1, planes):
        held = held + wout_recv[i].astype(F32)
    grad_out[...] = held
    for copy in terms:
        copy.wait_recv()
    for q in range(inner):
        for which in range(2):
            held = term_recv[which, q].astype(F32)
            for i in range(1, planes):
                held = held + term_recv[which, i * inner + q].astype(F32)
            at = (1 - which) * 2 * span
            grad_w[q, :, at : at + 2 * span] = held
    for copy in sent:
        copy.wait_send()


def fused_plan(activations, pair_repr, pair_gain, bias_weight, proj_weight, query_bias, out_weight, token_mask, out_cotangent):
    samples, tokens, feature = activations.shape
    tok = lax.axis_size("tok")
    cols, channels = pair_repr.shape[1:]
    group_heads = HEADS // INNER
    planes = tok // INNER
    span = group_heads * HD
    window = -(-span // 128) * 128
    shard = feature // tok
    total = INNER * tokens
    small_rows = HEADS + 16

    def vmem(*shape, dtype=BF16):
        return pltpu.VMEM(shape, dtype)

    def sems(*shape):
        return pltpu.SemaphoreType.DMA(shape)

    scratch = [
        vmem(feature, 4 * feature),
        vmem(span, feature),
        vmem(4, window, feature),
        vmem(INNER, tokens, feature),
        vmem(INNER, tokens, feature),
        vmem(feature, total),
        vmem(window, 128, dtype=F32),
        vmem(cols, tokens, channels, dtype=F32),
        vmem(cols, tokens, 1, dtype=F32),
        vmem(cols * HEADS, tokens, dtype=F32),
        vmem(INNER, group_heads, cols, tokens),
        vmem(tok, group_heads, cols, tokens),
    ]
    scratch += [vmem(group_heads, HD, total)] * 7
    scratch += [
        vmem(group_heads, INNER, tokens, tokens, dtype=F32),
        vmem(2, INNER, group_heads, HD, tokens),
        vmem(2, INNER, group_heads, HD, tokens),
        vmem(4, INNER, group_heads, HD, tokens),
        vmem(2, planes, INNER, shard, 2 * span),
        vmem(2, tok, shard, 2 * span),
        vmem(group_heads, HD, feature),
        vmem(planes, HD, feature),
        vmem(tok, group_heads, cols, tokens),
        vmem(tok, group_heads, cols, tokens),
        vmem(HEADS * cols, tokens, dtype=F32),
        vmem(HEADS + 24, channels, dtype=F32),
        vmem(small_rows, channels, dtype=F32),
        vmem(INNER, HEADS + 24, channels, dtype=F32),
        vmem(planes, small_rows, channels, dtype=F32),
        sems(2),
        sems(2, 6),
        sems(2, tok - 1),
        sems(2, 2 * tok),
        sems(2, max(planes, INNER)),
        sems(2, 2 * INNER),
        sems(2, tok - 1),
        sems(2, INNER + planes),
    ]
    in_vmem = pl.BlockSpec(memory_space=pltpu.VMEM)
    in_any = pl.BlockSpec(memory_space=pl.ANY)
    grad_act, grad_pair, grad_w, grad_out, small = pl.pallas_call(
        functools.partial(fused_kernel, tok),
        out_shape=[
            jax.ShapeDtypeStruct((tokens, feature), BF16),
            jax.ShapeDtypeStruct((cols, tokens, channels), BF16),
            jax.ShapeDtypeStruct((INNER, shard, 4 * span), F32),
            jax.ShapeDtypeStruct((shard, feature), F32),
            jax.ShapeDtypeStruct((small_rows, channels), F32),
        ],
        in_specs=[in_vmem] * 7 + [in_any] * 2,
        out_specs=[in_vmem] * 5,
        scratch_shapes=scratch,
        compiler_params=pltpu.CompilerParams(
            collective_id=3, has_side_effects=True, vmem_limit_bytes=48 * 2**20
        ),
        name="fused",
    )(
        activations.reshape(tokens, feature),
        out_cotangent.reshape(tokens, feature),
        pair_repr.transpose(1, 0, 2),
        pair_gain.reshape(1, channels),
        bias_weight.T,
        query_bias.reshape(1, feature),
        token_mask.reshape(1, tokens),
        proj_weight,
        out_weight,
    )
    grad_w = grad_w.reshape(INNER, shard, 4, span).transpose(1, 2, 0, 3).reshape(shard, 4 * feature)
    query_sums = small[HEADS + 8 :].reshape(INNER, window)[:, :span].reshape(feature)
    return (
        grad_act.reshape(samples, tokens, feature),
        grad_pair.transpose(1, 0, 2),
        grad_w,
        grad_out,
        query_sums,
        small[:HEADS].T,
        jnp.sum(small[HEADS : HEADS + 8], axis=0),
    )


def on_device(*args):
    samples, tokens, feature = args[0].shape
    tok = lax.axis_size("tok")
    cols, channels = args[1].shape[1:]
    square = tok == INNER * INNER and HEADS == tok and feature == HEADS * HD
    tiles = tokens == 128 and channels == 128 and tok * cols == tokens and cols % 8 == 0
    if samples == 1 and square and tiles:
        return fused_plan(*args)
    return general_plan(*args)


def solution(mesh):
    in_specs = (
        P(("groups", "tok"), None, None),
        P("groups", "tok", None),
        P(),
        P(),
        P(),
        P(),
        P(),
        P("groups"),
        P(("groups", "tok"), None, None),
    )
    out_specs = (
        P(("groups", "tok"), None, None),
        P("groups", "tok", None),
        P(("groups", "tok"), None),
        P(("groups", "tok"), None),
        P("groups"),
        P("groups", None),
        P("groups"),
    )
    return jax.shard_map(on_device, mesh=mesh, in_specs=in_specs, out_specs=out_specs, check_vma=False)
```

```python
import functools

import jax
import jax.numpy as jnp
from jax import lax
from jax.experimental import pallas as pl
from jax.experimental.pallas import tpu as pltpu
from jax.sharding import PartitionSpec as P

HEADS = 16
HD = 48
EPSILON = 1e-05
MASK_PENALTY = 10000.0
F32 = jnp.float32
BF16 = jnp.bfloat16
INNER = 4


def exchange_kernel(kinds, tok, *refs):
    count = len(kinds)
    ins, outs = refs[:count], refs[count : 2 * count]
    sends, recvs, local_sem = refs[2 * count : 3 * count], refs[3 * count : 4 * count], refs[4 * count]
    me = lax.axis_index("tok")
    group = me // INNER
    place = me % INNER
    across = place + 1 - 2 * (place % 2)
    beside = place + 2 - 4 * (place // 2)
    barrier = pltpu.get_barrier_semaphore()
    for step in range(1, tok):
        pl.semaphore_signal(barrier, inc=1, device_id={"tok": (me + step) % tok})
    pl.semaphore_wait(barrier, tok - 1)

    def send(k, slot, src, dst, peer):
        copy = pltpu.make_async_remote_copy(
            src_ref=src,
            dst_ref=dst,
            send_sem=sends[k].at[slot],
            recv_sem=recvs[k].at[slot],
            device_id={"tok": peer},
        )
        copy.start()
        return copy

    pending, relays, local = [], [], []
    for k, kind in enumerate(kinds):
        x, out = ins[k], outs[k]
        if kind == "near":
            first = send(k, 0, x, out.at[place], group * INNER + beside)
            pending.append(send(k, 1, x, out.at[place], group * INNER + across))
            relays.append((k, first, out.at[beside]))
        elif kind in ("all", "each"):
            for step in range(1, tok):
                peer = (me + step) % tok
                pending.append(send(k, step - 1, x if kind == "all" else x.at[peer], out.at[me], peer))
        elif kind == "near_each":
            for step in range(1, INNER):
                other = (place + step) % INNER
                pending.append(send(k, step - 1, x.at[other], out.at[place], group * INNER + other))
        else:
            for step in range(1, tok // INNER):
                other = (group + step) % (tok // INNER)
                pending.append(send(k, step - 1, x.at[other], out.at[group], other * INNER + place))
    for k, kind in enumerate(kinds):
        mine = {"all": me, "each": me, "near": place, "near_each": place, "far_each": group}[kind]
        own = ins[k] if kind in ("all", "near") else ins[k].at[mine]
        copy = pltpu.make_async_copy(own, outs[k].at[mine], local_sem.at[k])
        copy.start()
        local.append(copy)
    for k, first, block in relays:
        first.wait()
        pending.append(send(k, 2, block, block, group * INNER + across))
    for copy in local + pending:
        copy.wait()


def exchange(arrays, kinds, tok, collective_id):
    sizes = {"all": tok, "each": tok, "near": INNER, "near_each": INNER, "far_each": tok // INNER}
    shapes = []
    for x, kind in zip(arrays, kinds):
        block = x.shape if kind in ("all", "near") else x.shape[1:]
        shapes.append(jax.ShapeDtypeStruct((sizes[kind],) + block, x.dtype))
    sems = [pltpu.SemaphoreType.DMA((max(3, sizes[kind] - 1),)) for kind in kinds]
    return pl.pallas_call(
        functools.partial(exchange_kernel, kinds, tok),
        out_shape=shapes,
        in_specs=[pl.BlockSpec(memory_space=pltpu.VMEM)] * len(kinds),
        out_specs=[pl.BlockSpec(memory_space=pltpu.VMEM)] * len(kinds),
        scratch_shapes=sems + sems + [pltpu.SemaphoreType.DMA((len(kinds),))],
        compiler_params=pltpu.CompilerParams(
            collective_id=collective_id, has_side_effects=True, vmem_limit_bytes=40 * 2**20
        ),
        name=f"exchange_{collective_id}",
    )(*arrays)


def attention(query, keys, values, gate, grad_gated, bias_t, key_bias):
    scale = HD ** (-0.5)
    scores = jnp.einsum("hdj,hdi->hji", keys, query, preferred_element_type=F32) * scale
    scores = scores + bias_t.transpose(1, 0, 2).astype(F32) + key_bias[None, :, None]
    peak = jnp.max(scores, axis=1, keepdims=True)
    expo = jnp.exp(scores - peak)
    probs = expo / jnp.sum(expo, axis=1, keepdims=True)
    probs_b = probs.astype(BF16)
    attended = jnp.einsum("hdj,hji->hdi", values, probs_b, preferred_element_type=F32).astype(BF16)
    gate32 = gate.astype(F32)
    grad32 = grad_gated.astype(F32)
    att32 = attended.astype(F32)
    gated = (gate32 * att32).astype(BF16)
    grad_att = (grad32 * gate32).astype(BF16)
    grad_logit = (grad32 * att32 * gate32 * (1.0 - gate32)).astype(BF16)
    grad_probs = jnp.einsum("hdj,hdi->hji", values, grad_att, preferred_element_type=F32)
    grad_scores = probs * (grad_probs - jnp.sum(probs * grad_probs, axis=1, keepdims=True))
    scores_b = grad_scores.astype(BF16)
    grad_query = (jnp.einsum("hdj,hji->hdi", keys, scores_b, preferred_element_type=F32) * scale).astype(BF16)
    grad_key = (jnp.einsum("hdi,hji->hdj", query, scores_b, preferred_element_type=F32) * scale).astype(BF16)
    grad_value = jnp.einsum("hdi,hji->hdj", grad_att, probs_b, preferred_element_type=F32).astype(BF16)
    return jnp.stack([grad_query, grad_key, grad_value, grad_logit]), gated, grad_scores


def general_plan(activations, pair_repr, pair_gain, bias_weight, proj_weight, query_bias, out_weight, token_mask, out_cotangent):
    samples, tokens, feature = activations.shape
    tok = lax.axis_size("tok")
    cols = pair_repr.shape[1]
    act = activations.reshape(samples * tokens, feature)
    cot = out_cotangent.reshape(samples * tokens, feature)
    pair_f = pair_repr.astype(F32)
    centred = pair_f - jnp.mean(pair_f, axis=-1, keepdims=True)
    rstd = lax.rsqrt(jnp.mean(centred * centred, axis=-1, keepdims=True) + EPSILON)
    normed = centred * rstd
    scaled = normed * pair_gain
    bias_cols = jnp.einsum("ijc,ch->jhi", scaled, bias_weight, precision=lax.Precision.HIGHEST).astype(BF16)
    outer = tok // INNER
    shard = feature // tok

    def near_blocks(x):
        blocks = x.reshape(outer, INNER, shard, samples * tokens).transpose(1, 0, 2, 3)
        return blocks.reshape(INNER, outer * shard, samples * tokens)

    bias_t, cot_near, act_near = exchange(
        (bias_cols, cot, near_blocks(act.T)), ("all", "near", "near_each"), tok, 0
    )
    bias_t = bias_t.reshape((tok * cols,) + bias_cols.shape[1:])
    proj = jnp.einsum("tf,fn->nt", act, proj_weight, preferred_element_type=F32)
    proj = proj.reshape(4, feature, samples * tokens)
    query = (proj[0] + query_bias[:, None]).astype(BF16)
    keys = proj[1].astype(BF16)
    values = proj[2].astype(BF16)
    gate = jax.nn.sigmoid(proj[3]).astype(BF16)
    grad_gated = jnp.einsum("tn,mn->mt", cot, out_weight, preferred_element_type=F32).astype(BF16)
    key_bias = (token_mask.astype(F32) - 1.0) * MASK_PENALTY

    def heads_of(x):
        return x.reshape(HEADS, HD, samples, tokens).transpose(2, 0, 1, 3)

    grads, gated, grad_scores = jax.vmap(attention, in_axes=(0, 0, 0, 0, 0, None, None))(
        heads_of(query), heads_of(keys), heads_of(values), heads_of(gate), heads_of(grad_gated), bias_t, key_bias
    )
    grad_rows = grads.transpose(1, 2, 3, 0, 4).reshape(4 * feature, samples * tokens)
    gated_t = gated.transpose(1, 2, 0, 3).reshape(feature, samples * tokens)
    score_sum = jnp.sum(grad_scores, axis=0).astype(BF16)
    outgoing = score_sum.reshape(HEADS, tok, cols, tokens).transpose(1, 2, 0, 3)
    received, rows_near, gated_near = exchange(
        (outgoing, grad_rows, near_blocks(gated_t)), ("each", "near", "near_each"), tok, 1
    )
    grad_bias = jnp.sum(received.astype(F32), axis=0)
    grad_activations = jnp.einsum("nt,fn->tf", grad_rows, proj_weight, preferred_element_type=F32).astype(BF16)
    grad_zg = jnp.einsum("jhi,ch->ijc", grad_bias, bias_weight, precision=lax.Precision.HIGHEST)
    weight_part = jnp.einsum("ijc,jhi->ch", scaled, grad_bias, precision=lax.Precision.HIGHEST)
    gain_part = jnp.sum(normed * grad_zg, axis=(0, 1))
    query_part = jnp.sum(grad_rows[:feature].astype(F32), axis=1)
    small = jnp.concatenate([query_part, weight_part.reshape(-1), gain_part])
    small = jnp.pad(small, (0, -small.size % 1024)).reshape(-1, 128)
    first = jnp.einsum("srt,snt->rn", act_near, rows_near, preferred_element_type=F32)
    second = jnp.einsum("srt,stn->rn", gated_near, cot_near, preferred_element_type=F32)
    terms = jnp.concatenate([first.astype(BF16), second.astype(BF16)], axis=1)
    terms, small = exchange((terms.reshape(outer, shard, -1), small), ("far_each", "all"), tok, 2)
    weight_grads = jnp.sum(terms.astype(F32), axis=0)
    small = jnp.sum(small, axis=0).reshape(-1)
    grad_norm = grad_zg * pair_gain
    grad_pair = (
        grad_norm
        - jnp.mean(grad_norm, axis=-1, keepdims=True)
        - normed * jnp.mean(grad_norm * normed, axis=-1, keepdims=True)
    ) * rstd
    split = feature + weight_part.size
    return (
        grad_activations.reshape(samples, tokens, feature),
        grad_pair.astype(BF16),
        weight_grads[:, : 4 * feature],
        weight_grads[:, 4 * feature :],
        small[:feature],
        small[feature:split].reshape(weight_part.shape),
        small[split : split + pair_gain.shape[0]],
    )


NN = (((1,), (0,)), ((), ()))
NT = (((1,), (1,)), ((), ()))
TN = (((0,), (0,)), ((), ()))


def dot(a, b, dims, precision=None):
    return lax.dot_general(a, b, dims, precision=precision, preferred_element_type=F32)


def fused_kernel(
    tok,
    act,
    cot,
    pair_hbm,
    gain_hbm,
    bias_w,
    query_hbm,
    mask_hbm,
    proj_hbm,
    out_w_hbm,
    grad_act,
    grad_pair,
    grad_w,
    grad_out,
    query_out,
    small_out,
    gain_out,
    proj_w,
    out_w,
    pair,
    gain,
    query_bias,
    mask,
    proj_t,
    act_all,
    cot_all,
    act_t,
    query_col,
    normed,
    rstd,
    bias_f,
    bias_send,
    bias_recv,
    q_s,
    k_s,
    v_s,
    g_s,
    att_s,
    ga_s,
    gated_s,
    gg_send,
    gg_s,
    probs_s,
    rows_a,
    rows_b,
    rows_back,
    term_send,
    term_recv,
    wout_send,
    wout_recv,
    score_send,
    score_recv,
    score_f,
    pair_f,
    small_a,
    small_b,
    recv_a,
    recv_b,
    local_sem,
    act_sems,
    gg_sems,
    bias_sems,
    term_sems,
    wout_sems,
    back_sems,
    score_sems,
    small_sems,
):
    tokens, feature = act.shape
    inner = INNER
    planes = tok // inner
    group_heads, head_dim = q_s.shape[0], q_s.shape[1]
    cols = pair.shape[1]
    channels = pair.shape[2]
    span = group_heads * head_dim
    window = proj_t.shape[1]
    shard = feature // tok
    scale = head_dim ** (-0.5)
    me = lax.axis_index("tok")
    plane = me // inner
    place = me % inner
    across = place + 1 - 2 * (place % 2)
    beside = place + 2 - 4 * (place // 2)
    diagonal = across + 2 - 4 * (across // 2)
    base = pl.multiple_of((place * span) // 128 * 128, 128)
    offset = pl.multiple_of(place * span - (place * span) // 128 * 128, 64)

    def load(src, dst, slot):
        copy = pltpu.make_async_copy(src, dst, local_sem.at[slot])
        copy.start()
        return copy

    load_act = load(act, act_all.at[place], 0)
    load_pair = load(pair_hbm, pair, 1)
    load_cot = load(cot, cot_all.at[place], 2)
    load_small = [load(gain_hbm, gain, 3), load(query_hbm, query_bias, 4), load(mask_hbm, mask, 5)]
    load_out = load(out_w_hbm, out_w, 6)
    load_proj = load(proj_hbm, proj_w, 7)

    barrier = pltpu.get_barrier_semaphore()
    for step in range(1, tok):
        pl.semaphore_signal(barrier, inc=1, device_id={"tok": (me + step) % tok})

    def remote(src, dst, sems, slot, peer, arrival=None):
        return pltpu.make_async_remote_copy(
            src_ref=src,
            dst_ref=dst,
            send_sem=sems.at[0, slot],
            recv_sem=sems.at[1, slot if arrival is None else arrival],
            device_id={"tok": peer},
        )

    def near(where):
        return plane * inner + where

    sent = []
    load_pair.wait()
    for copy in load_small:
        copy.wait()
    gains = gain[...].reshape(1, channels)
    x = pair[...].astype(F32).reshape(tokens * cols, channels)
    centred = x - jnp.mean(x, axis=-1, keepdims=True)
    r = lax.rsqrt(jnp.mean(centred * centred, axis=-1, keepdims=True) + EPSILON)
    normed[...] = centred * r
    rstd[...] = jnp.broadcast_to(r, (tokens * cols, channels))
    for j in range(cols):
        y = normed[pl.ds(j, tokens, stride=cols), :]
        part = dot(bias_w[...], y * gains, NT, lax.Precision.HIGHEST)
        bias_f[pl.ds(j * HEADS, HEADS), :] = part
    for h in range(HEADS):
        bias_send[h // group_heads, h % group_heads] = bias_f[pl.ds(h, cols, stride=HEADS), :].astype(BF16)
    load_act.wait()
    pl.semaphore_wait(barrier, tok - 1)
    mine = act_all.at[place]
    act_beside = remote(mine, mine, act_sems, 0, near(beside))
    act_across = remote(mine, mine, act_sems, 1, near(across))
    for copy in (act_beside, act_across):
        copy.start()
        sent.append(copy)
    bias_copies = []
    for step in range(1, tok):
        peer = (me + step) % tok
        copy = remote(bias_send.at[peer % inner], bias_recv.at[me], bias_sems, step - 1, peer)
        copy.start()
        bias_copies.append(copy)
    sent += bias_copies
    load_cot.wait()
    load_out.wait()
    parts = dot(out_w[...], cot_all[place], NT).astype(BF16)
    gg_send[...] = parts.reshape(gg_send.shape)
    gg_copies = []
    for d in range(1, inner):
        where = (place + d) % inner
        copy = remote(gg_send.at[where], gg_s.at[place], gg_sems, d, near(where))
        copy.start()
        gg_copies.append(copy)
    sent += gg_copies
    mine = cot_all.at[place]
    cot_beside = remote(mine, mine, act_sems, 2, near(beside))
    cot_across = remote(mine, mine, act_sems, 3, near(across))
    for copy in (cot_beside, cot_across):
        copy.start()
        sent.append(copy)
    bias_recv[me] = bias_send[place]
    gg_s[place] = gg_send[place]

    shifts = query_bias[...].reshape(1, feature)
    row = jnp.broadcast_to(shifts, (128, feature))
    for c in range(feature // 128):
        query_col[c * 128 : (c + 1) * 128, :] = row[:, c * 128 : (c + 1) * 128].T
    load_proj.wait()
    for b in range(4):
        proj_t[b] = proj_w[:, pl.ds(pl.multiple_of(feature * b + base, 128), window)].T

    act_beside.wait_recv()
    act_relay = remote(act_all.at[beside], act_all.at[beside], act_sems, 4, near(across))
    act_relay.start()
    sent.append(act_relay)
    act_across.wait_recv()
    act_relay.wait_recv()
    total = inner * tokens
    acts = act_all[...].reshape(total, feature)
    stored = (group_heads, head_dim, total)
    for b, target in enumerate((q_s, k_s, v_s, g_s)):
        block = dot(proj_t[b, pl.ds(offset, span), :], acts, NT)
        if b == 0:
            shift = query_col[pl.ds(pl.multiple_of(place * span, 64), span), :]
            block = block + jnp.concatenate([shift] * (total // 128), axis=1)
        if b == 3:
            block = jax.nn.sigmoid(block)
        target[...] = block.astype(BF16).reshape(stored)
    for copy in bias_copies:
        copy.wait_recv()

    key_row = jnp.broadcast_to((mask[...].reshape(1, tokens).astype(F32) - 1.0) * MASK_PENALTY, (tokens, tokens))
    key_bias = key_row.T

    def forward(k, carry):
        bias = bias_recv[:, k].astype(F32).reshape(tokens, tokens)
        for s in range(inner):
            at = slice(s * tokens, (s + 1) * tokens)
            query, keys, values = q_s[k, :, at], k_s[k, :, at], v_s[k, :, at]
            scores = dot(keys, query, TN) * scale + bias + key_bias
            expo = jnp.exp(scores - jnp.max(scores, axis=0, keepdims=True))
            probs = expo / jnp.sum(expo, axis=0, keepdims=True)
            probs_s[k, s] = probs
            attended = dot(values, probs.astype(BF16), NN).astype(BF16)
            att_s[k, :, at] = attended
            gated_s[k, :, at] = (g_s[k, :, at].astype(F32) * attended.astype(F32)).astype(BF16)
        return carry

    lax.fori_loop(0, group_heads, forward, 0)
    for i in range(inner):
        act_t[:, i * tokens : (i + 1) * tokens] = act_all[i].T
    for copy in gg_copies:
        copy.wait_recv()

    def gates(k, carry):
        for s in range(inner):
            at = slice(s * tokens, (s + 1) * tokens)
            gate32 = g_s[k, :, at].astype(F32)
            grad32 = gg_s[s, k].astype(F32)
            attended = att_s[k, :, at].astype(F32)
            grad_att = (grad32 * gate32).astype(BF16)
            ga_s[k, :, at] = grad_att
            rows_a[1, s, k] = (grad32 * attended * gate32 * (1.0 - gate32)).astype(BF16)
            rows_a[0, s, k] = dot(grad_att, probs_s[k, s].astype(BF16), NT).astype(BF16)
        return carry

    lax.fori_loop(0, group_heads, gates, 0)
    cot_beside.wait_recv()
    cot_relay = remote(cot_all.at[beside], cot_all.at[beside], act_sems, 5, near(across))
    cot_relay.start()
    sent.append(cot_relay)

    order = [planes // 2] + [o for o in range(1, planes) if o != planes // 2] + [0]

    def send_terms(which, rows):
        for o in order:
            target = (plane + o) % planes
            lhs = act_t[pl.ds(pl.multiple_of(target * (inner * shard), 16), inner * shard), :]
            part = dot(lhs, rows, NT)
            term_send[which, target] = part.astype(BF16).reshape(inner, shard, 2 * span)
            for d in range(inner):
                if o == 0 and d == 0:
                    continue
                where = (place + d) % inner
                copy = remote(
                    term_send.at[which, target, where],
                    term_recv.at[which, me],
                    term_sems,
                    which * tok + o * inner + d,
                    target * inner + where,
                )
                copy.start()
                sent.append(copy)
                terms.append(copy)
        term_recv[which, me] = term_send[which, plane, place]

    def send_rows(which, rows):
        for d in range(1, inner):
            where = (place + d) % inner
            copy = remote(
                rows.at[:, where],
                rows_back.at[pl.ds(2 - 2 * which, 2), place],
                back_sems,
                which * inner + d,
                near(where),
            )
            copy.start()
            sent.append(copy)
            backs.append(copy)
        rows_back[pl.ds(2 - 2 * which, 2), place] = rows[:, place]

    def side_by_side(rows):
        return jnp.concatenate([rows[:, s].reshape(2 * span, tokens) for s in range(inner)], axis=1)

    terms, backs = [], []
    send_terms(0, side_by_side(rows_a))
    cot_across.wait_recv()
    cot_relay.wait_recv()
    cots = cot_all[...].reshape(total, feature)
    wout_send[...] = dot(gated_s[...].reshape(span, total), cots, NN).astype(BF16).reshape(wout_send.shape)
    wouts = []
    for d in range(inner):
        where = (place + d) % inner
        copy = remote(wout_send.at[where], wout_recv.at[plane], wout_sems, d, place * inner + where, plane)
        if d == 0:
            @pl.when(place != plane)
            def _():
                copy.start()

            @pl.when(place == plane)
            def _():
                wout_recv[plane] = wout_send[place]
        else:
            copy.start()
        wouts.append(copy)
    send_rows(0, rows_a)

    def backward(k, carry):
        summed = jnp.zeros((tokens, tokens), F32)
        for s in range(inner):
            at = slice(s * tokens, (s + 1) * tokens)
            query, keys, values = q_s[k, :, at], k_s[k, :, at], v_s[k, :, at]
            probs = probs_s[k, s]
            grad_probs = dot(values, ga_s[k, :, at], TN)
            grad_scores = probs * (grad_probs - jnp.sum(probs * grad_probs, axis=0, keepdims=True))
            scores_b = grad_scores.astype(BF16)
            rows_b[0, s, k] = (dot(keys, scores_b, NN) * scale).astype(BF16)
            rows_b[1, s, k] = (dot(query, scores_b, NT) * scale).astype(BF16)
            summed = summed + grad_scores
        score_send[:, k] = summed.reshape(tok, cols, tokens).astype(BF16)
        return carry

    lax.fori_loop(0, group_heads, backward, 0)

    scores = []
    for step in range(1, tok):
        peer = (me + step) % tok
        copy = remote(score_send.at[peer], score_recv.at[me], score_sems, step - 1, peer)
        copy.start()
        scores.append(copy)
    sent += scores
    score_recv[me] = score_send[me]
    send_rows(1, rows_b)
    rows = side_by_side(rows_b)
    send_terms(1, rows)
    query_part = dot(jnp.ones((8, total), BF16), rows[:window], NT)

    for copy in scores:
        copy.wait_recv()
    for q in range(inner):
        for k in range(group_heads):
            part = score_recv[q, k].astype(F32)
            for i in range(1, planes):
                part = part + score_recv[i * inner + q, k].astype(F32)
            h = q * group_heads + k
            score_f[pl.ds(h * cols, cols), :] = part
    weight_part = jnp.zeros((HEADS, channels), F32)
    gain_part = jnp.zeros((8, channels), F32)
    for j in range(cols):
        grad_bias = score_f[pl.ds(j, HEADS, stride=cols), :]
        y = normed[pl.ds(j, tokens, stride=cols), :]
        weight_part = weight_part + dot(grad_bias, y * gains, NN, lax.Precision.HIGHEST)
        grad_zg = dot(grad_bias, bias_w[...], TN, lax.Precision.HIGHEST)
        gain_part = gain_part + jnp.sum((y * grad_zg).reshape(tokens // 8, 8, channels), axis=0)
        g = grad_zg * gains
        first = jnp.mean(g, axis=-1, keepdims=True)
        second = jnp.mean(g * y, axis=-1, keepdims=True)
        pair_f[pl.ds(j, tokens, stride=cols), :] = (g - first - y * second) * rstd[pl.ds(j, tokens, stride=cols), :]
    grad_pair[...] = pair_f[...].reshape(tokens, cols, channels).astype(BF16)
    small_a[0:HEADS, :] = weight_part
    small_a[HEADS : HEADS + 8, :] = gain_part
    small_a[HEADS + 8 : HEADS + 16, :] = query_part[:, :128]
    small_a[HEADS + 16 : HEADS + 24, :] = query_part[:, 128:]
    firsts = []
    for d in range(1, inner):
        where = (place + d) % inner
        copy = remote(small_a, recv_a.at[place], small_sems, d, near(where))
        copy.start()
        firsts.append(copy)
    sent += firsts
    recv_a[place] = small_a[...]
    for copy in firsts:
        copy.wait_recv()
    held = recv_a[0, 0 : HEADS + 8, :]
    for q in range(1, inner):
        held = held + recv_a[q, 0 : HEADS + 8, :]
    small_b[0 : HEADS + 8, :] = held
    for q in range(inner):
        for half in range(2):
            at = HEADS + 8 + 8 * half
            small_b[HEADS + 8 + 2 * q + half : HEADS + 9 + 2 * q + half, :] = recv_a[q, at : at + 1, :]
    seconds = []
    for o in range(1, planes):
        target = (plane + o) % planes
        copy = remote(small_b, recv_b.at[plane], small_sems, inner + o, target * inner + place)
        copy.start()
        seconds.append(copy)
    sent += seconds
    recv_b[plane] = small_b[...]

    for copy in backs:
        copy.wait_recv()
    back = rows_back[...].reshape(4 * feature, tokens)
    for c in range(feature // 128):
        part = dot(proj_w[c * 128 : (c + 1) * 128, :], back, NN)
        grad_act[:, c * 128 : (c + 1) * 128] = part.T.astype(BF16)

    for copy in seconds:
        copy.wait_recv()
    held = recv_b[0]
    for i in range(1, planes):
        held = held + recv_b[i]
    small_out[...] = held[0:HEADS]
    gain_out[...] = jnp.sum(held[HEADS : HEADS + 8], axis=0)
    pieces = []
    for q in range(inner):
        at = HEADS + 8 + 2 * q
        pieces.append(jnp.concatenate([held[at : at + 1], held[at + 1 : at + 2, : span - 128]], axis=1))
    query_out[...] = jnp.concatenate(pieces, axis=1).reshape(feature)

    for d, copy in enumerate(wouts):
        if d == 0:
            @pl.when(place != plane)
            def _():
                copy.wait_send()
        else:
            copy.wait_send()
    for o in range(planes):
        source = (plane + o) % planes
        copy = remote(wout_send.at[0], wout_recv.at[source], wout_sems, 0, near(across), source)
        if o == 0:
            @pl.when(place != plane)
            def _():
                copy.wait_recv()
        else:
            copy.wait_recv()

    held = wout_recv[0].astype(F32)
    for i in range(1, planes):
        held = held + wout_recv[i].astype(F32)
    grad_out[...] = held
    for copy in terms:
        copy.wait_recv()
    for which in range(2):
        sums = []
        for q in range(inner):
            held = term_recv[which, q].astype(F32)
            for i in range(1, planes):
                held = held + term_recv[which, i * inner + q].astype(F32)
            sums.append(held)
        for b in range(2):
            at = (2 - 2 * which + b) * feature
            joined = jnp.concatenate([x[:, b * span : (b + 1) * span] for x in sums], axis=1)
            grad_w[:, at : at + feature] = joined
    for copy in sent:
        copy.wait_send()


def finish_kernel(*refs):
    count = len(refs) // 2
    ins, outs, sem = refs[:count], refs[count : 2 * count], refs[2 * count]
    copies = [pltpu.make_async_copy(ins[i], outs[i], sem.at[i]) for i in range(count)]
    for copy in copies:
        copy.start()
    for copy in copies:
        copy.wait()


def fused_plan(activations, pair_repr, pair_gain, bias_weight, proj_weight, query_bias, out_weight, token_mask, out_cotangent):
    samples, tokens, feature = activations.shape
    tok = lax.axis_size("tok")
    cols, channels = pair_repr.shape[1:]
    group_heads = HEADS // INNER
    planes = tok // INNER
    span = group_heads * HD
    window = -(-span // 128) * 128
    shard = feature // tok
    total = INNER * tokens
    small_rows = HEADS + 16

    def vmem(*shape, dtype=BF16):
        return pltpu.VMEM(shape, dtype)

    def sems(*shape):
        return pltpu.SemaphoreType.DMA(shape)

    scratch = [
        vmem(feature, 4 * feature),
        vmem(feature, feature),
        vmem(tokens, cols, channels),
        vmem(channels, dtype=F32),
        vmem(feature, dtype=F32),
        vmem(tokens, dtype=jnp.int32),
        vmem(4, window, feature),
        vmem(INNER, tokens, feature),
        vmem(INNER, tokens, feature),
        vmem(feature, total),
        vmem(feature, 128, dtype=F32),
        vmem(tokens * cols, channels, dtype=F32),
        vmem(tokens * cols, channels, dtype=F32),
        vmem(cols * HEADS, tokens, dtype=F32),
        vmem(INNER, group_heads, cols, tokens),
        vmem(tok, group_heads, cols, tokens),
    ]
    scratch += [vmem(group_heads, HD, total)] * 7
    scratch += [
        vmem(INNER, group_heads, HD, tokens),
        vmem(INNER, group_heads, HD, tokens),
        vmem(group_heads, INNER, tokens, tokens, dtype=F32),
        vmem(2, INNER, group_heads, HD, tokens),
        vmem(2, INNER, group_heads, HD, tokens),
        vmem(4, INNER, group_heads, HD, tokens),
        vmem(2, planes, INNER, shard, 2 * span),
        vmem(2, tok, shard, 2 * span),
        vmem(group_heads, HD, feature),
        vmem(planes, HD, feature),
        vmem(tok, group_heads, cols, tokens),
        vmem(tok, group_heads, cols, tokens),
        vmem(HEADS * cols, tokens, dtype=F32),
        vmem(tokens * cols, channels, dtype=F32),
        vmem(HEADS + 24, channels, dtype=F32),
        vmem(small_rows, channels, dtype=F32),
        vmem(INNER, HEADS + 24, channels, dtype=F32),
        vmem(planes, small_rows, channels, dtype=F32),
        sems(8),
        sems(2, 6),
        sems(2, INNER),
        sems(2, tok - 1),
        sems(2, 2 * tok),
        sems(2, max(planes, INNER)),
        sems(2, 2 * INNER),
        sems(2, tok - 1),
        sems(2, INNER + planes),
    ]
    in_vmem = pl.BlockSpec(memory_space=pltpu.VMEM)
    in_hbm = pl.BlockSpec(memory_space=pltpu.HBM)
    shapes = [
        jax.ShapeDtypeStruct((tokens, feature), BF16),
        jax.ShapeDtypeStruct((tokens, cols, channels), BF16),
        jax.ShapeDtypeStruct((shard, 4 * feature), F32),
        jax.ShapeDtypeStruct((shard, feature), F32),
        jax.ShapeDtypeStruct((feature,), F32),
        jax.ShapeDtypeStruct((HEADS, channels), F32),
        jax.ShapeDtypeStruct((channels,), F32),
    ]
    results = pl.pallas_call(
        functools.partial(fused_kernel, tok),
        out_shape=shapes,
        in_specs=[in_hbm] * 4 + [in_vmem] + [in_hbm] * 4,
        out_specs=[in_vmem] * len(shapes),
        scratch_shapes=scratch,
        compiler_params=pltpu.CompilerParams(
            collective_id=3, has_side_effects=True, vmem_limit_bytes=67043328
        ),
        name="fused",
    )(
        activations.reshape(tokens, feature),
        out_cotangent.reshape(tokens, feature),
        pair_repr,
        pair_gain,
        bias_weight.T,
        query_bias,
        token_mask,
        proj_weight,
        out_weight,
    )
    results = pl.pallas_call(
        finish_kernel,
        out_shape=shapes,
        in_specs=[in_vmem] * len(shapes),
        out_specs=[in_hbm] * len(shapes),
        scratch_shapes=[pltpu.SemaphoreType.DMA((len(shapes),))],
        name="finish",
    )(*results)
    grad_act, grad_pair, grad_w, grad_out, query_sums, weight_sums, gain_sums = results
    return (
        grad_act.reshape(samples, tokens, feature),
        grad_pair,
        grad_w,
        grad_out,
        query_sums,
        weight_sums.T,
        gain_sums,
    )


def on_device(*args):
    samples, tokens, feature = args[0].shape
    tok = lax.axis_size("tok")
    cols, channels = args[1].shape[1:]
    square = tok == INNER * INNER and HEADS == tok and feature == HEADS * HD
    tiles = tokens == 128 and channels == 128 and tok * cols == tokens and cols % 8 == 0
    if samples == 1 and square and tiles:
        return fused_plan(*args)
    return general_plan(*args)


def solution(mesh):
    in_specs = (
        P(("groups", "tok"), None, None),
        P("groups", "tok", None),
        P(),
        P(),
        P(),
        P(),
        P(),
        P("groups"),
        P(("groups", "tok"), None, None),
    )
    out_specs = (
        P(("groups", "tok"), None, None),
        P("groups", "tok", None),
        P(("groups", "tok"), None),
        P(("groups", "tok"), None),
        P("groups"),
        P("groups", None),
        P("groups"),
    )
    return jax.shard_map(on_device, mesh=mesh, in_specs=in_specs, out_specs=out_specs, check_vma=False)
```

```python
import functools

import jax
import jax.numpy as jnp
from jax import lax
from jax.experimental import pallas as pl
from jax.experimental.pallas import tpu as pltpu
from jax.sharding import PartitionSpec as P

HEADS = 16
HD = 48
EPSILON = 1e-05
MASK_PENALTY = 10000.0
F32 = jnp.float32
BF16 = jnp.bfloat16
INNER = 4


def exchange_kernel(kinds, tok, *refs):
    count = len(kinds)
    ins, outs = refs[:count], refs[count : 2 * count]
    sends, recvs, local_sem = refs[2 * count : 3 * count], refs[3 * count : 4 * count], refs[4 * count]
    me = lax.axis_index("tok")
    group = me // INNER
    place = me % INNER
    across = place + 1 - 2 * (place % 2)
    beside = place + 2 - 4 * (place // 2)
    barrier = pltpu.get_barrier_semaphore()
    for step in range(1, tok):
        pl.semaphore_signal(barrier, inc=1, device_id={"tok": (me + step) % tok})
    pl.semaphore_wait(barrier, tok - 1)

    def send(k, slot, src, dst, peer):
        copy = pltpu.make_async_remote_copy(
            src_ref=src,
            dst_ref=dst,
            send_sem=sends[k].at[slot],
            recv_sem=recvs[k].at[slot],
            device_id={"tok": peer},
        )
        copy.start()
        return copy

    pending, relays, local = [], [], []
    for k, kind in enumerate(kinds):
        x, out = ins[k], outs[k]
        if kind == "near":
            first = send(k, 0, x, out.at[place], group * INNER + beside)
            pending.append(send(k, 1, x, out.at[place], group * INNER + across))
            relays.append((k, first, out.at[beside]))
        elif kind in ("all", "each"):
            for step in range(1, tok):
                peer = (me + step) % tok
                pending.append(send(k, step - 1, x if kind == "all" else x.at[peer], out.at[me], peer))
        elif kind == "near_each":
            for step in range(1, INNER):
                other = (place + step) % INNER
                pending.append(send(k, step - 1, x.at[other], out.at[place], group * INNER + other))
        else:
            for step in range(1, tok // INNER):
                other = (group + step) % (tok // INNER)
                pending.append(send(k, step - 1, x.at[other], out.at[group], other * INNER + place))
    for k, kind in enumerate(kinds):
        mine = {"all": me, "each": me, "near": place, "near_each": place, "far_each": group}[kind]
        own = ins[k] if kind in ("all", "near") else ins[k].at[mine]
        copy = pltpu.make_async_copy(own, outs[k].at[mine], local_sem.at[k])
        copy.start()
        local.append(copy)
    for k, first, block in relays:
        first.wait()
        pending.append(send(k, 2, block, block, group * INNER + across))
    for copy in local + pending:
        copy.wait()


def exchange(arrays, kinds, tok, collective_id):
    sizes = {"all": tok, "each": tok, "near": INNER, "near_each": INNER, "far_each": tok // INNER}
    shapes = []
    for x, kind in zip(arrays, kinds):
        block = x.shape if kind in ("all", "near") else x.shape[1:]
        shapes.append(jax.ShapeDtypeStruct((sizes[kind],) + block, x.dtype))
    sems = [pltpu.SemaphoreType.DMA((max(3, sizes[kind] - 1),)) for kind in kinds]
    return pl.pallas_call(
        functools.partial(exchange_kernel, kinds, tok),
        out_shape=shapes,
        in_specs=[pl.BlockSpec(memory_space=pltpu.VMEM)] * len(kinds),
        out_specs=[pl.BlockSpec(memory_space=pltpu.VMEM)] * len(kinds),
        scratch_shapes=sems + sems + [pltpu.SemaphoreType.DMA((len(kinds),))],
        compiler_params=pltpu.CompilerParams(
            collective_id=collective_id, has_side_effects=True, vmem_limit_bytes=40 * 2**20
        ),
        name=f"exchange_{collective_id}",
    )(*arrays)


def attention(query, keys, values, gate, grad_gated, bias_t, key_bias):
    scale = HD ** (-0.5)
    scores = jnp.einsum("hdj,hdi->hji", keys, query, preferred_element_type=F32) * scale
    scores = scores + bias_t.transpose(1, 0, 2).astype(F32) + key_bias[None, :, None]
    peak = jnp.max(scores, axis=1, keepdims=True)
    expo = jnp.exp(scores - peak)
    probs = expo / jnp.sum(expo, axis=1, keepdims=True)
    probs_b = probs.astype(BF16)
    attended = jnp.einsum("hdj,hji->hdi", values, probs_b, preferred_element_type=F32).astype(BF16)
    gate32 = gate.astype(F32)
    grad32 = grad_gated.astype(F32)
    att32 = attended.astype(F32)
    gated = (gate32 * att32).astype(BF16)
    grad_att = (grad32 * gate32).astype(BF16)
    grad_logit = (grad32 * att32 * gate32 * (1.0 - gate32)).astype(BF16)
    grad_probs = jnp.einsum("hdj,hdi->hji", values, grad_att, preferred_element_type=F32)
    grad_scores = probs * (grad_probs - jnp.sum(probs * grad_probs, axis=1, keepdims=True))
    scores_b = grad_scores.astype(BF16)
    grad_query = (jnp.einsum("hdj,hji->hdi", keys, scores_b, preferred_element_type=F32) * scale).astype(BF16)
    grad_key = (jnp.einsum("hdi,hji->hdj", query, scores_b, preferred_element_type=F32) * scale).astype(BF16)
    grad_value = jnp.einsum("hdi,hji->hdj", grad_att, probs_b, preferred_element_type=F32).astype(BF16)
    return jnp.stack([grad_query, grad_key, grad_value, grad_logit]), gated, grad_scores


def general_plan(activations, pair_repr, pair_gain, bias_weight, proj_weight, query_bias, out_weight, token_mask, out_cotangent):
    samples, tokens, feature = activations.shape
    tok = lax.axis_size("tok")
    cols = pair_repr.shape[1]
    act = activations.reshape(samples * tokens, feature)
    cot = out_cotangent.reshape(samples * tokens, feature)
    pair_f = pair_repr.astype(F32)
    centred = pair_f - jnp.mean(pair_f, axis=-1, keepdims=True)
    rstd = lax.rsqrt(jnp.mean(centred * centred, axis=-1, keepdims=True) + EPSILON)
    normed = centred * rstd
    scaled = normed * pair_gain
    bias_cols = jnp.einsum("ijc,ch->jhi", scaled, bias_weight, precision=lax.Precision.HIGHEST).astype(BF16)
    outer = tok // INNER
    shard = feature // tok

    def near_blocks(x):
        blocks = x.reshape(outer, INNER, shard, samples * tokens).transpose(1, 0, 2, 3)
        return blocks.reshape(INNER, outer * shard, samples * tokens)

    bias_t, cot_near, act_near = exchange(
        (bias_cols, cot, near_blocks(act.T)), ("all", "near", "near_each"), tok, 0
    )
    bias_t = bias_t.reshape((tok * cols,) + bias_cols.shape[1:])
    proj = jnp.einsum("tf,fn->nt", act, proj_weight, preferred_element_type=F32)
    proj = proj.reshape(4, feature, samples * tokens)
    query = (proj[0] + query_bias[:, None]).astype(BF16)
    keys = proj[1].astype(BF16)
    values = proj[2].astype(BF16)
    gate = jax.nn.sigmoid(proj[3]).astype(BF16)
    grad_gated = jnp.einsum("tn,mn->mt", cot, out_weight, preferred_element_type=F32).astype(BF16)
    key_bias = (token_mask.astype(F32) - 1.0) * MASK_PENALTY

    def heads_of(x):
        return x.reshape(HEADS, HD, samples, tokens).transpose(2, 0, 1, 3)

    grads, gated, grad_scores = jax.vmap(attention, in_axes=(0, 0, 0, 0, 0, None, None))(
        heads_of(query), heads_of(keys), heads_of(values), heads_of(gate), heads_of(grad_gated), bias_t, key_bias
    )
    grad_rows = grads.transpose(1, 2, 3, 0, 4).reshape(4 * feature, samples * tokens)
    gated_t = gated.transpose(1, 2, 0, 3).reshape(feature, samples * tokens)
    score_sum = jnp.sum(grad_scores, axis=0).astype(BF16)
    outgoing = score_sum.reshape(HEADS, tok, cols, tokens).transpose(1, 2, 0, 3)
    received, rows_near, gated_near = exchange(
        (outgoing, grad_rows, near_blocks(gated_t)), ("each", "near", "near_each"), tok, 1
    )
    grad_bias = jnp.sum(received.astype(F32), axis=0)
    grad_activations = jnp.einsum("nt,fn->tf", grad_rows, proj_weight, preferred_element_type=F32).astype(BF16)
    grad_zg = jnp.einsum("jhi,ch->ijc", grad_bias, bias_weight, precision=lax.Precision.HIGHEST)
    weight_part = jnp.einsum("ijc,jhi->ch", scaled, grad_bias, precision=lax.Precision.HIGHEST)
    gain_part = jnp.sum(normed * grad_zg, axis=(0, 1))
    query_part = jnp.sum(grad_rows[:feature].astype(F32), axis=1)
    small = jnp.concatenate([query_part, weight_part.reshape(-1), gain_part])
    small = jnp.pad(small, (0, -small.size % 1024)).reshape(-1, 128)
    first = jnp.einsum("srt,snt->rn", act_near, rows_near, preferred_element_type=F32)
    second = jnp.einsum("srt,stn->rn", gated_near, cot_near, preferred_element_type=F32)
    terms = jnp.concatenate([first.astype(BF16), second.astype(BF16)], axis=1)
    terms, small = exchange((terms.reshape(outer, shard, -1), small), ("far_each", "all"), tok, 2)
    weight_grads = jnp.sum(terms.astype(F32), axis=0)
    small = jnp.sum(small, axis=0).reshape(-1)
    grad_norm = grad_zg * pair_gain
    grad_pair = (
        grad_norm
        - jnp.mean(grad_norm, axis=-1, keepdims=True)
        - normed * jnp.mean(grad_norm * normed, axis=-1, keepdims=True)
    ) * rstd
    split = feature + weight_part.size
    return (
        grad_activations.reshape(samples, tokens, feature),
        grad_pair.astype(BF16),
        weight_grads[:, : 4 * feature],
        weight_grads[:, 4 * feature :],
        small[:feature],
        small[feature:split].reshape(weight_part.shape),
        small[split : split + pair_gain.shape[0]],
    )


NN = (((1,), (0,)), ((), ()))
NT = (((1,), (1,)), ((), ()))
TN = (((0,), (0,)), ((), ()))


def dot(a, b, dims, precision=None):
    return lax.dot_general(a, b, dims, precision=precision, preferred_element_type=F32)


def fused_kernel(
    tok,
    act,
    cot,
    pair_hbm,
    gain_hbm,
    bias_w,
    query_hbm,
    mask_hbm,
    proj_hbm,
    out_w_hbm,
    grad_act,
    grad_pair,
    grad_w,
    grad_out,
    query_out,
    small_out,
    gain_out,
    proj_w,
    out_w,
    pair,
    gain,
    query_bias,
    mask,
    proj_t,
    act_all,
    cot_all,
    act_t,
    query_col,
    normed,
    rstd,
    bias_f,
    bias_send,
    bias_recv,
    q_s,
    k_s,
    v_s,
    g_s,
    att_s,
    ga_s,
    gated_s,
    gg_send,
    gg_s,
    probs_s,
    rows_a,
    rows_b,
    back_part,
    back_send,
    back_recv,
    term_send,
    term_hop,
    term_end,
    wout_send,
    wout_hop,
    wout_end,
    score_send,
    score_recv,
    score_f,
    pair_f,
    small_a,
    small_b,
    recv_a,
    recv_b,
    local_sem,
    act_sems,
    gg_sems,
    bias_sems,
    term_sems,
    wout_sems,
    back_sems,
    score_sems,
    small_sems,
):
    tokens, feature = act.shape
    inner = INNER
    planes = tok // inner
    group_heads, head_dim = q_s.shape[0], q_s.shape[1]
    cols = pair.shape[1]
    channels = pair.shape[2]
    span = group_heads * head_dim
    window = proj_t.shape[1]
    shard = feature // tok
    scale = head_dim ** (-0.5)
    me = lax.axis_index("tok")
    plane = me // inner
    place = me % inner
    across = place + 1 - 2 * (place % 2)
    beside = place + 2 - 4 * (place // 2)
    diagonal = across + 2 - 4 * (across // 2)
    base = pl.multiple_of((place * span) // 128 * 128, 128)
    offset = pl.multiple_of(place * span - (place * span) // 128 * 128, 64)

    def load(src, dst, slot):
        copy = pltpu.make_async_copy(src, dst, local_sem.at[slot])
        copy.start()
        return copy

    load_act = load(act, act_all.at[place], 0)
    load_pair = load(pair_hbm, pair, 1)
    load_cot = load(cot, cot_all.at[place], 2)
    load_small = [load(gain_hbm, gain, 3), load(query_hbm, query_bias, 4), load(mask_hbm, mask, 5)]
    load_out = load(out_w_hbm, out_w, 6)
    load_proj = [
        load(proj_hbm.at[:, pl.ds(pl.multiple_of(feature * b + base, 128), window)], proj_w.at[b], 7 + b)
        for b in range(4)
    ]

    barrier = pltpu.get_barrier_semaphore()
    for step in range(1, tok):
        pl.semaphore_signal(barrier, inc=1, device_id={"tok": (me + step) % tok})

    def remote(src, dst, sems, slot, peer, arrival=None):
        return pltpu.make_async_remote_copy(
            src_ref=src,
            dst_ref=dst,
            send_sem=sems.at[0, slot],
            recv_sem=sems.at[1, slot if arrival is None else arrival],
            device_id={"tok": peer},
        )

    def near(where):
        return plane * inner + where

    sent = []
    load_pair.wait()
    for copy in load_small:
        copy.wait()
    gains = gain[...].reshape(1, channels)
    x = pair[...].astype(F32).reshape(tokens * cols, channels)
    centred = x - jnp.mean(x, axis=-1, keepdims=True)
    r = lax.rsqrt(jnp.mean(centred * centred, axis=-1, keepdims=True) + EPSILON)
    normed[...] = centred * r
    rstd[...] = jnp.broadcast_to(r, (tokens * cols, channels))
    for j in range(cols):
        y = normed[pl.ds(j, tokens, stride=cols), :]
        part = dot(bias_w[...], y * gains, NT, lax.Precision.HIGHEST)
        bias_f[pl.ds(j * HEADS, HEADS), :] = part
    for h in range(HEADS):
        bias_send[h // group_heads, h % group_heads] = bias_f[pl.ds(h, cols, stride=HEADS), :].astype(BF16)
    load_act.wait()
    pl.semaphore_wait(barrier, tok - 1)
    mine = act_all.at[place]
    act_beside = remote(mine, mine, act_sems, 0, near(beside))
    act_across = remote(mine, mine, act_sems, 1, near(across))
    for copy in (act_beside, act_across):
        copy.start()
        sent.append(copy)
    bias_copies = []
    for step in range(1, tok):
        peer = (me + step) % tok
        copy = remote(bias_send.at[peer % inner], bias_recv.at[me], bias_sems, step - 1, peer)
        copy.start()
        bias_copies.append(copy)
    sent += bias_copies
    load_cot.wait()
    load_out.wait()
    parts = dot(out_w[...], cot_all[place], NT).astype(BF16)
    gg_send[...] = parts.reshape(gg_send.shape)
    gg_copies = []
    for d in range(1, inner):
        where = (place + d) % inner
        copy = remote(gg_send.at[where], gg_s.at[place], gg_sems, d, near(where))
        copy.start()
        gg_copies.append(copy)
    sent += gg_copies
    mine = cot_all.at[place]
    cot_beside = remote(mine, mine, act_sems, 2, near(beside))
    cot_across = remote(mine, mine, act_sems, 3, near(across))
    for copy in (cot_beside, cot_across):
        copy.start()
        sent.append(copy)
    bias_recv[me] = bias_send[place]
    gg_s[place] = gg_send[place]

    shifts = query_bias[...].reshape(1, feature)
    row = jnp.broadcast_to(shifts, (128, feature))
    for c in range(feature // 128):
        query_col[c * 128 : (c + 1) * 128, :] = row[:, c * 128 : (c + 1) * 128].T
    for b in range(4):
        load_proj[b].wait()
        proj_t[b] = proj_w[b].T

    act_beside.wait_recv()
    act_relay = remote(act_all.at[beside], act_all.at[beside], act_sems, 4, near(across))
    act_relay.start()
    sent.append(act_relay)
    act_across.wait_recv()
    act_relay.wait_recv()
    total = inner * tokens
    acts = act_all[...].reshape(total, feature)
    stored = (group_heads, head_dim, total)
    for b, target in enumerate((q_s, k_s, v_s, g_s)):
        block = dot(proj_t[b, pl.ds(offset, span), :], acts, NT)
        if b == 0:
            shift = query_col[pl.ds(pl.multiple_of(place * span, 64), span), :]
            block = block + jnp.concatenate([shift] * (total // 128), axis=1)
        if b == 3:
            block = jax.nn.sigmoid(block)
        target[...] = block.astype(BF16).reshape(stored)
    for copy in bias_copies:
        copy.wait_recv()

    key_row = jnp.broadcast_to((mask[...].reshape(1, tokens).astype(F32) - 1.0) * MASK_PENALTY, (tokens, tokens))
    key_bias = key_row.T

    def forward(k, carry):
        bias = bias_recv[:, k].astype(F32).reshape(tokens, tokens)
        for s in range(inner):
            at = slice(s * tokens, (s + 1) * tokens)
            query, keys, values = q_s[k, :, at], k_s[k, :, at], v_s[k, :, at]
            scores = dot(keys, query, TN) * scale + bias + key_bias
            expo = jnp.exp(scores - jnp.max(scores, axis=0, keepdims=True))
            probs = expo / jnp.sum(expo, axis=0, keepdims=True)
            probs_s[k, s] = probs
            attended = dot(values, probs.astype(BF16), NN).astype(BF16)
            att_s[k, :, at] = attended
            gated_s[k, :, at] = (g_s[k, :, at].astype(F32) * attended.astype(F32)).astype(BF16)
        return carry

    lax.fori_loop(0, group_heads, forward, 0)
    for i in range(inner):
        act_t[:, i * tokens : (i + 1) * tokens] = act_all[i].T
    for copy in gg_copies:
        copy.wait_recv()

    def gates(k, carry):
        for s in range(inner):
            at = slice(s * tokens, (s + 1) * tokens)
            gate32 = g_s[k, :, at].astype(F32)
            grad32 = gg_s[s, k].astype(F32)
            attended = att_s[k, :, at].astype(F32)
            grad_att = (grad32 * gate32).astype(BF16)
            ga_s[k, :, at] = grad_att
            rows_a[1, s, k] = (grad32 * attended * gate32 * (1.0 - gate32)).astype(BF16)
            rows_a[0, s, k] = dot(grad_att, probs_s[k, s].astype(BF16), NT).astype(BF16)
        return carry

    lax.fori_loop(0, group_heads, gates, 0)
    cot_beside.wait_recv()
    cot_relay = remote(cot_all.at[beside], cot_all.at[beside], act_sems, 5, near(across))
    cot_relay.start()
    sent.append(cot_relay)

    lane_sems = planes + inner
    ends = (plane == 0) | (plane == planes - 1)
    neighbour = jnp.where(plane < planes // 2, plane + 1, plane - 1)

    def turn(i):
        return jnp.where(plane < planes // 2, planes - 1 - i, i)

    def move_terms(which, target, act_on):
        up = target > plane
        following = jnp.where(up, plane + 1, plane - 1)
        way = jnp.where(up, 0, 1)
        first = (which * 3 + way) * lane_sems

        @pl.when(following == target)
        def _():
            for d in range(inner):
                where = (place + d) % inner
                act_on(
                    remote(
                        term_send.at[which, target, where],
                        term_end.at[which, way, place],
                        term_sems,
                        first + planes + d,
                        following * inner + where,
                        first + planes + place,
                    )
                )

        @pl.when(following != target)
        def _():
            act_on(
                remote(
                    term_send.at[which, target],
                    term_hop.at[which, target],
                    term_sems,
                    first + target,
                    following * inner + place,
                )
            )

    def start(copy):
        copy.start()

    def send_terms(which, rows):
        for i in range(planes):
            target = turn(i)
            lhs = act_t[pl.ds(pl.multiple_of(target * (inner * shard), 16), inner * shard), :]
            part = dot(lhs, rows, NT)
            term_send[which, target] = part.astype(BF16).reshape(inner, shard, 2 * span)

            @pl.when(ends & (target != plane) & (target != neighbour))
            def _():
                move_terms(which, target, start)

        first = (which * 3 + 2) * lane_sems + planes
        for d in range(1, inner):
            where = (place + d) % inner
            copy = remote(
                term_send.at[which, plane, where],
                term_end.at[which, 2, place],
                term_sems,
                first + d,
                near(where),
                first + place,
            )
            copy.start()
            sent.append(copy)
        term_end[which, 2, place] = term_send[which, plane, place]

    def relay_terms(which, i):
        target = turn(i)

        @pl.when(jnp.logical_not(ends) & (target != plane))
        def _():
            way = jnp.where(target > plane, 0, 1)
            slot = (which * 3 + way) * lane_sems + target
            remote(
                term_send.at[which, target], term_hop.at[which, target], term_sems, slot, near(across)
            ).wait_recv()
            held = term_send[which, target].astype(F32) + term_hop[which, target].astype(F32)
            term_send[which, target] = held.astype(BF16)
            move_terms(which, target, start)

    def settle_terms(which):
        for i in range(planes):
            target = turn(i)

            @pl.when(target != plane)
            def _():
                move_terms(which, target, lambda copy: copy.wait_send())

    def ended_terms(which, way):
        first = (which * 3 + way) * lane_sems + planes
        for q in range(inner):
            copy = remote(
                term_send.at[which, 0, 0], term_end.at[which, way, q], term_sems, 0, near(across), first + q
            )
            if way == 2:
                pl.when(place != q)(copy.wait_recv)
            else:
                copy.wait_recv()

    def late_terms(which):
        @pl.when(ends)
        def _():
            move_terms(which, neighbour, start)

    def move_wout(k, act_on):
        up = place > plane
        following = jnp.where(up, plane + 1, plane - 1)
        way = jnp.where(up, 0, 1)

        @pl.when((place != plane) & (following == place))
        def _():
            act_on(remote(wout_send.at[k], wout_end.at[way], wout_sems, 3 + k, following * inner + k, way))

        @pl.when((place != plane) & (following != place))
        def _():
            act_on(remote(wout_send.at[k], wout_hop.at[k], wout_sems, 3 + k, following * inner + place))

        @pl.when((place == plane) & (place != k))
        def _():
            act_on(remote(wout_send.at[k], wout_end.at[2], wout_sems, 3 + k, near(k), 2))

    def relay_wout(k):
        @pl.when(jnp.logical_not(wout_first))
        def _():
            remote(wout_send.at[k], wout_hop.at[k], wout_sems, 3 + k, near(across)).wait_recv()
            wout_send[k] = (wout_send[k].astype(F32) + wout_hop[k].astype(F32)).astype(BF16)
            move_wout(k, start)

    def side_by_side(rows):
        return jnp.concatenate([rows[:, s].reshape(2 * span, tokens) for s in range(inner)], axis=1)

    send_terms(0, side_by_side(rows_a))
    cot_across.wait_recv()
    cot_relay.wait_recv()
    cots = cot_all[...].reshape(total, feature)
    wout_send[...] = dot(gated_s[...].reshape(span, total), cots, NN).astype(BF16).reshape(wout_send.shape)

    @pl.when(place == plane)
    def _():
        wout_end[2] = wout_send[place]

    wout_first = ends | (place == plane)


    def backward(k, carry):
        summed = jnp.zeros((tokens, tokens), F32)
        for s in range(inner):
            at = slice(s * tokens, (s + 1) * tokens)
            query, keys, values = q_s[k, :, at], k_s[k, :, at], v_s[k, :, at]
            probs = probs_s[k, s]
            grad_probs = dot(values, ga_s[k, :, at], TN)
            grad_scores = probs * (grad_probs - jnp.sum(probs * grad_probs, axis=0, keepdims=True))
            scores_b = grad_scores.astype(BF16)
            rows_b[0, s, k] = (dot(keys, scores_b, NN) * scale).astype(BF16)
            rows_b[1, s, k] = (dot(query, scores_b, NT) * scale).astype(BF16)
            summed = summed + grad_scores
        score_send[:, k] = summed.reshape(tok, cols, tokens).astype(BF16)
        return carry

    lax.fori_loop(0, group_heads, backward, 0)

    scores = []
    for step in range(1, tok):
        peer = (me + step) % tok
        copy = remote(score_send.at[peer], score_recv.at[me], score_sems, step - 1, peer)
        copy.start()
        scores.append(copy)
    sent += scores
    score_recv[me] = score_send[me]
    relay_terms(0, 0)
    relay_terms(0, 1)
    rows = side_by_side(rows_b)
    send_terms(1, rows)

    @pl.when(wout_first)
    def _():
        for k in range(group_heads):
            move_wout(k, start)

    for i in range(2, planes):
        relay_terms(0, i)
    query_part = dot(jnp.ones((8, total), BF16), rows[:window], NT)

    for copy in scores:
        copy.wait_recv()
    for q in range(inner):
        for k in range(group_heads):
            part = score_recv[q, k].astype(F32)
            for i in range(1, planes):
                part = part + score_recv[i * inner + q, k].astype(F32)
            h = q * group_heads + k
            score_f[pl.ds(h * cols, cols), :] = part
    weight_part = jnp.zeros((HEADS, channels), F32)
    gain_part = jnp.zeros((8, channels), F32)
    for j in range(cols):
        grad_bias = score_f[pl.ds(j, HEADS, stride=cols), :]
        y = normed[pl.ds(j, tokens, stride=cols), :]
        weight_part = weight_part + dot(grad_bias, y * gains, NN, lax.Precision.HIGHEST)
        grad_zg = dot(grad_bias, bias_w[...], TN, lax.Precision.HIGHEST)
        gain_part = gain_part + jnp.sum((y * grad_zg).reshape(tokens // 8, 8, channels), axis=0)
        g = grad_zg * gains
        first = jnp.mean(g, axis=-1, keepdims=True)
        second = jnp.mean(g * y, axis=-1, keepdims=True)
        pair_f[pl.ds(j, tokens, stride=cols), :] = (g - first - y * second) * rstd[pl.ds(j, tokens, stride=cols), :]
    grad_pair[...] = pair_f[...].reshape(tokens, cols, channels).astype(BF16)
    small_a[0:HEADS, :] = weight_part
    small_a[HEADS : HEADS + 8, :] = gain_part
    small_a[HEADS + 8 : HEADS + 16, :] = query_part[:, :128]
    small_a[HEADS + 16 : HEADS + 24, :] = query_part[:, 128:]
    firsts = []
    for d in range(1, inner):
        where = (place + d) % inner
        copy = remote(small_a, recv_a.at[place], small_sems, d, near(where))
        copy.start()
        firsts.append(copy)
    sent += firsts
    recv_a[place] = small_a[...]
    for copy in firsts:
        copy.wait_recv()
    held = recv_a[0, 0 : HEADS + 8, :]
    for q in range(1, inner):
        held = held + recv_a[q, 0 : HEADS + 8, :]
    small_b[0 : HEADS + 8, :] = held
    for q in range(inner):
        for half in range(2):
            at = HEADS + 8 + 8 * half
            small_b[HEADS + 8 + 2 * q + half : HEADS + 9 + 2 * q + half, :] = recv_a[q, at : at + 1, :]
    seconds = []
    for o in range(1, planes):
        target = (plane + o) % planes
        copy = remote(small_b, recv_b.at[plane], small_sems, inner + o, target * inner + place)
        copy.start()
        seconds.append(copy)
    sent += seconds
    recv_b[plane] = small_b[...]

    late_terms(0)
    late_terms(1)
    relay_terms(1, 0)
    relay_terms(1, 1)
    weights = jnp.concatenate([proj_t[b, pl.ds(offset, span), :] for b in range(4)], axis=0)

    def back_of(first, second):
        columns = []
        for s in (first, second):
            both = [x[:, s].reshape(2 * span, tokens) for x in (rows_b, rows_a)]
            columns.append(jnp.concatenate(both, axis=0))
        return dot(jnp.concatenate(columns, axis=1), weights, TN)

    back_send[0:2] = back_of(diagonal, across).astype(BF16).reshape(2, tokens, feature)
    backs = [remote(back_send.at[i], back_recv.at[i], back_sems, i, near(across)) for i in range(2)]
    for copy in backs:
        copy.start()
    back_part[...] = back_of(beside, place).reshape(2, tokens, feature)
    backs[0].wait_recv()
    back_send[2] = (back_part[0] + back_recv[0].astype(F32)).astype(BF16)
    backs.append(remote(back_send.at[2], back_recv.at[2], back_sems, 2, near(beside)))
    backs[2].start()
    sent += backs
    for i in range(2, planes):
        relay_terms(1, i)
    for k in range(group_heads):
        relay_wout(k)
    for copy in seconds:
        copy.wait_recv()
    held = recv_b[0]
    for i in range(1, planes):
        held = held + recv_b[i]
    small_out[...] = held[0:HEADS]
    gain_out[...] = jnp.sum(held[HEADS : HEADS + 8], axis=0)
    pieces = []
    for q in range(inner):
        at = HEADS + 8 + 2 * q
        pieces.append(jnp.concatenate([held[at : at + 1], held[at + 1 : at + 2, : span - 128]], axis=1))
    query_out[...] = jnp.concatenate(pieces, axis=1).reshape(feature)

    for copy in backs[1:]:
        copy.wait_recv()
    held = back_part[1] + back_recv[1].astype(F32) + back_recv[2].astype(F32)
    grad_act[...] = held.astype(BF16)

    def ended_wout(way):
        remote(wout_send.at[0], wout_end.at[way], wout_sems, 0, near(across), way).wait_recv()

    pl.when(plane > 0)(lambda: ended_wout(0))
    pl.when(plane < planes - 1)(lambda: ended_wout(1))
    pl.when(place != plane)(lambda: ended_wout(2))
    grad_out[...] = wout_end[2].astype(F32)

    @pl.when(plane > 0)
    def _():
        grad_out[...] += wout_end[0].astype(F32)

    @pl.when(plane < planes - 1)
    def _():
        grad_out[...] += wout_end[1].astype(F32)

    for which in range(2):
        ended_terms(which, 2)
        pl.when(plane > 0)(lambda: ended_terms(which, 0))
        pl.when(plane < planes - 1)(lambda: ended_terms(which, 1))
        sums = []
        for q in range(inner):
            held = term_end[which, 2, q].astype(F32)
            for there, way in ((plane > 0, 0), (plane < planes - 1, 1)):
                held = held + jnp.where(there, term_end[which, way, q].astype(F32), 0.0)
            sums.append(held)
        for b in range(2):
            at = (2 - 2 * which + b) * feature
            joined = jnp.concatenate([x[:, b * span : (b + 1) * span] for x in sums], axis=1)
            grad_w[:, at : at + feature] = joined
    for copy in sent:
        copy.wait_send()
    for k in range(group_heads):
        move_wout(k, lambda copy: copy.wait_send())
    for which in range(2):
        settle_terms(which)


def finish_kernel(*refs):
    count = len(refs) // 2
    ins, outs, sem = refs[:count], refs[count : 2 * count], refs[2 * count]
    copies = [pltpu.make_async_copy(ins[i], outs[i], sem.at[i]) for i in range(count)]
    for copy in copies:
        copy.start()
    for copy in copies:
        copy.wait()


def fused_plan(activations, pair_repr, pair_gain, bias_weight, proj_weight, query_bias, out_weight, token_mask, out_cotangent):
    samples, tokens, feature = activations.shape
    tok = lax.axis_size("tok")
    cols, channels = pair_repr.shape[1:]
    group_heads = HEADS // INNER
    planes = tok // INNER
    span = group_heads * HD
    window = -(-span // 128) * 128
    shard = feature // tok
    total = INNER * tokens
    small_rows = HEADS + 16

    def vmem(*shape, dtype=BF16):
        return pltpu.VMEM(shape, dtype)

    def sems(*shape):
        return pltpu.SemaphoreType.DMA(shape)

    scratch = [
        vmem(4, feature, window),
        vmem(feature, feature),
        vmem(tokens, cols, channels),
        vmem(channels, dtype=F32),
        vmem(feature, dtype=F32),
        vmem(tokens, dtype=jnp.int32),
        vmem(4, window, feature),
        vmem(INNER, tokens, feature),
        vmem(INNER, tokens, feature),
        vmem(feature, total),
        vmem(feature, 128, dtype=F32),
        vmem(tokens * cols, channels, dtype=F32),
        vmem(tokens * cols, channels, dtype=F32),
        vmem(cols * HEADS, tokens, dtype=F32),
        vmem(INNER, group_heads, cols, tokens),
        vmem(tok, group_heads, cols, tokens),
    ]
    scratch += [vmem(group_heads, HD, total)] * 7
    scratch += [
        vmem(INNER, group_heads, HD, tokens),
        vmem(INNER, group_heads, HD, tokens),
        vmem(group_heads, INNER, tokens, tokens, dtype=F32),
        vmem(2, INNER, group_heads, HD, tokens),
        vmem(2, INNER, group_heads, HD, tokens),
        vmem(2, tokens, feature, dtype=F32),
        vmem(3, tokens, feature),
        vmem(3, tokens, feature),
        vmem(2, planes, INNER, shard, 2 * span),
        vmem(2, planes, INNER, shard, 2 * span),
        vmem(2, 3, INNER, shard, 2 * span),
        vmem(group_heads, HD, feature),
        vmem(group_heads, HD, feature),
        vmem(3, HD, feature),
        vmem(tok, group_heads, cols, tokens),
        vmem(tok, group_heads, cols, tokens),
        vmem(HEADS * cols, tokens, dtype=F32),
        vmem(tokens * cols, channels, dtype=F32),
        vmem(HEADS + 24, channels, dtype=F32),
        vmem(small_rows, channels, dtype=F32),
        vmem(INNER, HEADS + 24, channels, dtype=F32),
        vmem(planes, small_rows, channels, dtype=F32),
        sems(11),
        sems(2, 6),
        sems(2, INNER),
        sems(2, tok - 1),
        sems(2, 6 * (planes + INNER)),
        sems(2, 3 + group_heads),
        sems(2, 3),
        sems(2, tok - 1),
        sems(2, INNER + planes),
    ]
    in_vmem = pl.BlockSpec(memory_space=pltpu.VMEM)
    in_hbm = pl.BlockSpec(memory_space=pltpu.HBM)
    shapes = [
        jax.ShapeDtypeStruct((tokens, feature), BF16),
        jax.ShapeDtypeStruct((tokens, cols, channels), BF16),
        jax.ShapeDtypeStruct((shard, 4 * feature), F32),
        jax.ShapeDtypeStruct((shard, feature), F32),
        jax.ShapeDtypeStruct((feature,), F32),
        jax.ShapeDtypeStruct((HEADS, channels), F32),
        jax.ShapeDtypeStruct((channels,), F32),
    ]
    results = pl.pallas_call(
        functools.partial(fused_kernel, tok),
        out_shape=shapes,
        in_specs=[in_hbm] * 4 + [in_vmem] + [in_hbm] * 4,
        out_specs=[in_vmem] * len(shapes),
        scratch_shapes=scratch,
        compiler_params=pltpu.CompilerParams(
            collective_id=3, has_side_effects=True, vmem_limit_bytes=67043328
        ),
        name="fused",
    )(
        activations.reshape(tokens, feature),
        out_cotangent.reshape(tokens, feature),
        pair_repr,
        pair_gain,
        bias_weight.T,
        query_bias,
        token_mask,
        proj_weight,
        out_weight,
    )
    results = pl.pallas_call(
        finish_kernel,
        out_shape=shapes,
        in_specs=[in_vmem] * len(shapes),
        out_specs=[in_hbm] * len(shapes),
        scratch_shapes=[pltpu.SemaphoreType.DMA((len(shapes),))],
        name="finish",
    )(*results)
    grad_act, grad_pair, grad_w, grad_out, query_sums, weight_sums, gain_sums = results
    return (
        grad_act.reshape(samples, tokens, feature),
        grad_pair,
        grad_w,
        grad_out,
        query_sums,
        weight_sums.T,
        gain_sums,
    )


def on_device(*args):
    samples, tokens, feature = args[0].shape
    tok = lax.axis_size("tok")
    cols, channels = args[1].shape[1:]
    square = tok == INNER * INNER and HEADS == tok and feature == HEADS * HD
    tiles = tokens == 128 and channels == 128 and tok * cols == tokens and cols % 8 == 0
    if samples == 1 and square and tiles:
        return fused_plan(*args)
    return general_plan(*args)


def solution(mesh):
    in_specs = (
        P(("groups", "tok"), None, None),
        P("groups", "tok", None),
        P(),
        P(),
        P(),
        P(),
        P(),
        P("groups"),
        P(("groups", "tok"), None, None),
    )
    out_specs = (
        P(("groups", "tok"), None, None),
        P("groups", "tok", None),
        P(("groups", "tok"), None),
        P(("groups", "tok"), None),
        P("groups"),
        P("groups", None),
        P("groups"),
    )
    return jax.shard_map(on_device, mesh=mesh, in_specs=in_specs, out_specs=out_specs, check_vma=False)
```

```python
import functools

import jax
import jax.numpy as jnp
from jax import lax
from jax.experimental import pallas as pl
from jax.experimental.pallas import tpu as pltpu
from jax.sharding import PartitionSpec as P

HEADS = 16
HD = 48
EPSILON = 1e-05
MASK_PENALTY = 10000.0
F32 = jnp.float32
BF16 = jnp.bfloat16
INNER = 4


def exchange_kernel(kinds, tok, *refs):
    count = len(kinds)
    ins, outs = refs[:count], refs[count : 2 * count]
    sends, recvs, local_sem = refs[2 * count : 3 * count], refs[3 * count : 4 * count], refs[4 * count]
    me = lax.axis_index("tok")
    group = me // INNER
    place = me % INNER
    across = place + 1 - 2 * (place % 2)
    beside = place + 2 - 4 * (place // 2)
    barrier = pltpu.get_barrier_semaphore()
    for step in range(1, tok):
        pl.semaphore_signal(barrier, inc=1, device_id={"tok": (me + step) % tok})
    pl.semaphore_wait(barrier, tok - 1)

    def send(k, slot, src, dst, peer):
        copy = pltpu.make_async_remote_copy(
            src_ref=src,
            dst_ref=dst,
            send_sem=sends[k].at[slot],
            recv_sem=recvs[k].at[slot],
            device_id={"tok": peer},
        )
        copy.start()
        return copy

    pending, relays, local = [], [], []
    for k, kind in enumerate(kinds):
        x, out = ins[k], outs[k]
        if kind == "near":
            first = send(k, 0, x, out.at[place], group * INNER + beside)
            pending.append(send(k, 1, x, out.at[place], group * INNER + across))
            relays.append((k, first, out.at[beside]))
        elif kind in ("all", "each"):
            for step in range(1, tok):
                peer = (me + step) % tok
                pending.append(send(k, step - 1, x if kind == "all" else x.at[peer], out.at[me], peer))
        elif kind == "near_each":
            for step in range(1, INNER):
                other = (place + step) % INNER
                pending.append(send(k, step - 1, x.at[other], out.at[place], group * INNER + other))
        else:
            for step in range(1, tok // INNER):
                other = (group + step) % (tok // INNER)
                pending.append(send(k, step - 1, x.at[other], out.at[group], other * INNER + place))
    for k, kind in enumerate(kinds):
        mine = {"all": me, "each": me, "near": place, "near_each": place, "far_each": group}[kind]
        own = ins[k] if kind in ("all", "near") else ins[k].at[mine]
        copy = pltpu.make_async_copy(own, outs[k].at[mine], local_sem.at[k])
        copy.start()
        local.append(copy)
    for k, first, block in relays:
        first.wait()
        pending.append(send(k, 2, block, block, group * INNER + across))
    for copy in local + pending:
        copy.wait()


def exchange(arrays, kinds, tok, collective_id):
    sizes = {"all": tok, "each": tok, "near": INNER, "near_each": INNER, "far_each": tok // INNER}
    shapes = []
    for x, kind in zip(arrays, kinds):
        block = x.shape if kind in ("all", "near") else x.shape[1:]
        shapes.append(jax.ShapeDtypeStruct((sizes[kind],) + block, x.dtype))
    sems = [pltpu.SemaphoreType.DMA((max(3, sizes[kind] - 1),)) for kind in kinds]
    return pl.pallas_call(
        functools.partial(exchange_kernel, kinds, tok),
        out_shape=shapes,
        in_specs=[pl.BlockSpec(memory_space=pltpu.VMEM)] * len(kinds),
        out_specs=[pl.BlockSpec(memory_space=pltpu.VMEM)] * len(kinds),
        scratch_shapes=sems + sems + [pltpu.SemaphoreType.DMA((len(kinds),))],
        compiler_params=pltpu.CompilerParams(
            collective_id=collective_id, has_side_effects=True, vmem_limit_bytes=40 * 2**20
        ),
        name=f"exchange_{collective_id}",
    )(*arrays)


def attention(query, keys, values, gate, grad_gated, bias_t, key_bias):
    scale = HD ** (-0.5)
    scores = jnp.einsum("hdj,hdi->hji", keys, query, preferred_element_type=F32) * scale
    scores = scores + bias_t.transpose(1, 0, 2).astype(F32) + key_bias[None, :, None]
    peak = jnp.max(scores, axis=1, keepdims=True)
    expo = jnp.exp(scores - peak)
    probs = expo / jnp.sum(expo, axis=1, keepdims=True)
    probs_b = probs.astype(BF16)
    attended = jnp.einsum("hdj,hji->hdi", values, probs_b, preferred_element_type=F32).astype(BF16)
    gate32 = gate.astype(F32)
    grad32 = grad_gated.astype(F32)
    att32 = attended.astype(F32)
    gated = (gate32 * att32).astype(BF16)
    grad_att = (grad32 * gate32).astype(BF16)
    grad_logit = (grad32 * att32 * gate32 * (1.0 - gate32)).astype(BF16)
    grad_probs = jnp.einsum("hdj,hdi->hji", values, grad_att, preferred_element_type=F32)
    grad_scores = probs * (grad_probs - jnp.sum(probs * grad_probs, axis=1, keepdims=True))
    scores_b = grad_scores.astype(BF16)
    grad_query = (jnp.einsum("hdj,hji->hdi", keys, scores_b, preferred_element_type=F32) * scale).astype(BF16)
    grad_key = (jnp.einsum("hdi,hji->hdj", query, scores_b, preferred_element_type=F32) * scale).astype(BF16)
    grad_value = jnp.einsum("hdi,hji->hdj", grad_att, probs_b, preferred_element_type=F32).astype(BF16)
    return jnp.stack([grad_query, grad_key, grad_value, grad_logit]), gated, grad_scores


def general_plan(activations, pair_repr, pair_gain, bias_weight, proj_weight, query_bias, out_weight, token_mask, out_cotangent):
    samples, tokens, feature = activations.shape
    tok = lax.axis_size("tok")
    cols = pair_repr.shape[1]
    act = activations.reshape(samples * tokens, feature)
    cot = out_cotangent.reshape(samples * tokens, feature)
    pair_f = pair_repr.astype(F32)
    centred = pair_f - jnp.mean(pair_f, axis=-1, keepdims=True)
    rstd = lax.rsqrt(jnp.mean(centred * centred, axis=-1, keepdims=True) + EPSILON)
    normed = centred * rstd
    scaled = normed * pair_gain
    bias_cols = jnp.einsum("ijc,ch->jhi", scaled, bias_weight, precision=lax.Precision.HIGHEST).astype(BF16)
    outer = tok // INNER
    shard = feature // tok

    def near_blocks(x):
        blocks = x.reshape(outer, INNER, shard, samples * tokens).transpose(1, 0, 2, 3)
        return blocks.reshape(INNER, outer * shard, samples * tokens)

    bias_t, cot_near, act_near = exchange(
        (bias_cols, cot, near_blocks(act.T)), ("all", "near", "near_each"), tok, 0
    )
    bias_t = bias_t.reshape((tok * cols,) + bias_cols.shape[1:])
    proj = jnp.einsum("tf,fn->nt", act, proj_weight, preferred_element_type=F32)
    proj = proj.reshape(4, feature, samples * tokens)
    query = (proj[0] + query_bias[:, None]).astype(BF16)
    keys = proj[1].astype(BF16)
    values = proj[2].astype(BF16)
    gate = jax.nn.sigmoid(proj[3]).astype(BF16)
    grad_gated = jnp.einsum("tn,mn->mt", cot, out_weight, preferred_element_type=F32).astype(BF16)
    key_bias = (token_mask.astype(F32) - 1.0) * MASK_PENALTY

    def heads_of(x):
        return x.reshape(HEADS, HD, samples, tokens).transpose(2, 0, 1, 3)

    grads, gated, grad_scores = jax.vmap(attention, in_axes=(0, 0, 0, 0, 0, None, None))(
        heads_of(query), heads_of(keys), heads_of(values), heads_of(gate), heads_of(grad_gated), bias_t, key_bias
    )
    grad_rows = grads.transpose(1, 2, 3, 0, 4).reshape(4 * feature, samples * tokens)
    gated_t = gated.transpose(1, 2, 0, 3).reshape(feature, samples * tokens)
    score_sum = jnp.sum(grad_scores, axis=0).astype(BF16)
    outgoing = score_sum.reshape(HEADS, tok, cols, tokens).transpose(1, 2, 0, 3)
    received, rows_near, gated_near = exchange(
        (outgoing, grad_rows, near_blocks(gated_t)), ("each", "near", "near_each"), tok, 1
    )
    grad_bias = jnp.sum(received.astype(F32), axis=0)
    grad_activations = jnp.einsum("nt,fn->tf", grad_rows, proj_weight, preferred_element_type=F32).astype(BF16)
    grad_zg = jnp.einsum("jhi,ch->ijc", grad_bias, bias_weight, precision=lax.Precision.HIGHEST)
    weight_part = jnp.einsum("ijc,jhi->ch", scaled, grad_bias, precision=lax.Precision.HIGHEST)
    gain_part = jnp.sum(normed * grad_zg, axis=(0, 1))
    query_part = jnp.sum(grad_rows[:feature].astype(F32), axis=1)
    small = jnp.concatenate([query_part, weight_part.reshape(-1), gain_part])
    small = jnp.pad(small, (0, -small.size % 1024)).reshape(-1, 128)
    first = jnp.einsum("srt,snt->rn", act_near, rows_near, preferred_element_type=F32)
    second = jnp.einsum("srt,stn->rn", gated_near, cot_near, preferred_element_type=F32)
    terms = jnp.concatenate([first.astype(BF16), second.astype(BF16)], axis=1)
    terms, small = exchange((terms.reshape(outer, shard, -1), small), ("far_each", "all"), tok, 2)
    weight_grads = jnp.sum(terms.astype(F32), axis=0)
    small = jnp.sum(small, axis=0).reshape(-1)
    grad_norm = grad_zg * pair_gain
    grad_pair = (
        grad_norm
        - jnp.mean(grad_norm, axis=-1, keepdims=True)
        - normed * jnp.mean(grad_norm * normed, axis=-1, keepdims=True)
    ) * rstd
    split = feature + weight_part.size
    return (
        grad_activations.reshape(samples, tokens, feature),
        grad_pair.astype(BF16),
        weight_grads[:, : 4 * feature],
        weight_grads[:, 4 * feature :],
        small[:feature],
        small[feature:split].reshape(weight_part.shape),
        small[split : split + pair_gain.shape[0]],
    )


NN = (((1,), (0,)), ((), ()))
NT = (((1,), (1,)), ((), ()))
TN = (((0,), (0,)), ((), ()))


def dot(a, b, dims, precision=None):
    return lax.dot_general(a, b, dims, precision=precision, preferred_element_type=F32)


def fused_kernel(
    tok,
    act,
    cot,
    pair_hbm,
    gain_hbm,
    bias_w,
    query_hbm,
    mask_hbm,
    proj_hbm,
    out_w_hbm,
    grad_act,
    grad_pair,
    grad_w,
    grad_out,
    query_out,
    small_out,
    gain_out,
    proj_w,
    out_w,
    pair,
    gain,
    query_bias,
    mask,
    proj_t,
    act_all,
    cot_all,
    act_t,
    query_col,
    normed,
    rstd,
    bias_f,
    bias_send,
    bias_recv,
    q_s,
    k_s,
    v_s,
    g_s,
    att_s,
    ga_s,
    gated_s,
    gg_send,
    gg_s,
    probs_s,
    rows_a,
    rows_b,
    back_part,
    back_send,
    back_recv,
    term_send,
    term_hop,
    term_end,
    wout_send,
    wout_hop,
    wout_end,
    score_send,
    score_recv,
    score_f,
    pair_f,
    small_a,
    small_b,
    recv_a,
    recv_b,
    local_sem,
    act_sems,
    gg_sems,
    bias_sems,
    term_sems,
    wout_sems,
    back_sems,
    score_sems,
    small_sems,
):
    tokens, feature = act.shape
    inner = INNER
    planes = tok // inner
    group_heads, head_dim = q_s.shape[0], q_s.shape[1]
    cols = pair.shape[1]
    channels = pair.shape[2]
    span = group_heads * head_dim
    window = proj_t.shape[1]
    shard = feature // tok
    scale = head_dim ** (-0.5)
    me = lax.axis_index("tok")
    plane = me // inner
    place = me % inner
    across = place + 1 - 2 * (place % 2)
    beside = place + 2 - 4 * (place // 2)
    diagonal = across + 2 - 4 * (across // 2)
    base = pl.multiple_of((place * span) // 128 * 128, 128)
    offset = pl.multiple_of(place * span - (place * span) // 128 * 128, 64)

    def load(src, dst, slot):
        copy = pltpu.make_async_copy(src, dst, local_sem.at[slot])
        copy.start()
        return copy

    load_act = load(act, act_all.at[place], 0)
    load_pair = load(pair_hbm, pair, 1)
    load_cot = load(cot, cot_all.at[place], 2)
    load_small = [load(gain_hbm, gain, 3), load(query_hbm, query_bias, 4), load(mask_hbm, mask, 5)]
    load_out = load(out_w_hbm, out_w, 6)
    load_proj = [
        load(proj_hbm.at[:, pl.ds(pl.multiple_of(feature * b + base, 128), window)], proj_w.at[b], 7 + b)
        for b in range(4)
    ]

    barrier = pltpu.get_barrier_semaphore()
    for step in range(1, tok):
        pl.semaphore_signal(barrier, inc=1, device_id={"tok": (me + step) % tok})

    def remote(src, dst, sems, slot, peer, arrival=None):
        return pltpu.make_async_remote_copy(
            src_ref=src,
            dst_ref=dst,
            send_sem=sems.at[0, slot],
            recv_sem=sems.at[1, slot if arrival is None else arrival],
            device_id={"tok": peer},
        )

    def near(where):
        return plane * inner + where

    sent = []
    load_pair.wait()
    for copy in load_small:
        copy.wait()
    gains = gain[...].reshape(1, channels)
    x = pair[...].astype(F32).reshape(tokens * cols, channels)
    centred = x - jnp.mean(x, axis=-1, keepdims=True)
    r = lax.rsqrt(jnp.mean(centred * centred, axis=-1, keepdims=True) + EPSILON)
    normed[...] = centred * r
    rstd[...] = jnp.broadcast_to(r, (tokens * cols, channels))
    for j in range(cols):
        y = normed[pl.ds(j, tokens, stride=cols), :]
        part = dot(bias_w[...], y * gains, NT, lax.Precision.HIGHEST)
        bias_f[pl.ds(j * HEADS, HEADS), :] = part
    for h in range(HEADS):
        bias_send[h // group_heads, h % group_heads] = bias_f[pl.ds(h, cols, stride=HEADS), :].astype(BF16)
    load_act.wait()
    pl.semaphore_wait(barrier, tok - 1)
    mine = act_all.at[place]
    act_beside = remote(mine, mine, act_sems, 0, near(beside))
    act_across = remote(mine, mine, act_sems, 1, near(across))
    for copy in (act_beside, act_across):
        copy.start()
        sent.append(copy)
    bias_copies = []
    for step in range(1, tok):
        peer = (me + step) % tok
        copy = remote(bias_send.at[peer % inner], bias_recv.at[me], bias_sems, step - 1, peer)
        copy.start()
        bias_copies.append(copy)
    sent += bias_copies
    load_cot.wait()
    load_out.wait()
    parts = dot(out_w[...], cot_all[place], NT).astype(BF16)
    gg_send[...] = parts.reshape(gg_send.shape)
    gg_copies = []
    for d in range(1, inner):
        where = (place + d) % inner
        copy = remote(gg_send.at[where], gg_s.at[place], gg_sems, d, near(where))
        copy.start()
        gg_copies.append(copy)
    sent += gg_copies
    mine = cot_all.at[place]
    cot_beside = remote(mine, mine, act_sems, 2, near(beside))
    cot_across = remote(mine, mine, act_sems, 3, near(across))
    for copy in (cot_beside, cot_across):
        copy.start()
        sent.append(copy)
    bias_recv[me] = bias_send[place]
    gg_s[place] = gg_send[place]

    shifts = query_bias[...].reshape(1, feature)
    row = jnp.broadcast_to(shifts, (128, feature))
    for c in range(feature // 128):
        query_col[c * 128 : (c + 1) * 128, :] = row[:, c * 128 : (c + 1) * 128].T
    for b in range(4):
        load_proj[b].wait()
        proj_t[b] = proj_w[b].T

    act_beside.wait_recv()
    act_relay = remote(act_all.at[beside], act_all.at[beside], act_sems, 4, near(across))
    act_relay.start()
    sent.append(act_relay)
    act_across.wait_recv()
    act_relay.wait_recv()
    total = inner * tokens
    acts = act_all[...].reshape(total, feature)
    stored = (group_heads, head_dim, total)
    for b, target in enumerate((q_s, k_s, v_s, g_s)):
        block = dot(proj_t[b, pl.ds(offset, span), :], acts, NT)
        if b == 0:
            shift = query_col[pl.ds(pl.multiple_of(place * span, 64), span), :]
            block = block + jnp.concatenate([shift] * (total // 128), axis=1)
        if b == 3:
            block = jax.nn.sigmoid(block)
        target[...] = block.astype(BF16).reshape(stored)
    for copy in bias_copies:
        copy.wait_recv()

    key_row = jnp.broadcast_to((mask[...].reshape(1, tokens).astype(F32) - 1.0) * MASK_PENALTY, (tokens, tokens))
    key_bias = key_row.T

    def forward(k, carry):
        bias = bias_recv[:, k].astype(F32).reshape(tokens, tokens)
        for s in range(inner):
            at = slice(s * tokens, (s + 1) * tokens)
            query, keys, values = q_s[k, :, at], k_s[k, :, at], v_s[k, :, at]
            scores = dot(keys, query, TN) * scale + bias + key_bias
            expo = jnp.exp(scores - jnp.max(scores, axis=0, keepdims=True))
            probs = expo / jnp.sum(expo, axis=0, keepdims=True)
            probs_s[k, s] = probs
            attended = dot(values, probs.astype(BF16), NN).astype(BF16)
            att_s[k, :, at] = attended
            gated_s[k, :, at] = (g_s[k, :, at].astype(F32) * attended.astype(F32)).astype(BF16)
        return carry

    lax.fori_loop(0, group_heads, forward, 0)
    for i in range(inner):
        act_t[:, i * tokens : (i + 1) * tokens] = act_all[i].T
    for copy in gg_copies:
        copy.wait_recv()

    def gates(k, carry):
        for s in range(inner):
            at = slice(s * tokens, (s + 1) * tokens)
            gate32 = g_s[k, :, at].astype(F32)
            grad32 = gg_s[s, k].astype(F32)
            attended = att_s[k, :, at].astype(F32)
            grad_att = (grad32 * gate32).astype(BF16)
            ga_s[k, :, at] = grad_att
            rows_a[1, s, k] = (grad32 * attended * gate32 * (1.0 - gate32)).astype(BF16)
            rows_a[0, s, k] = dot(grad_att, probs_s[k, s].astype(BF16), NT).astype(BF16)
        return carry

    lax.fori_loop(0, group_heads, gates, 0)
    cot_beside.wait_recv()
    cot_relay = remote(cot_all.at[beside], cot_all.at[beside], act_sems, 5, near(across))
    cot_relay.start()
    sent.append(cot_relay)

    lane_sems = planes + inner
    ends = (plane == 0) | (plane == planes - 1)
    neighbour = jnp.where(plane < planes // 2, plane + 1, plane - 1)

    def turn(i):
        return jnp.where(plane < planes // 2, planes - 1 - i, i)

    def move_terms(which, target, act_on):
        up = target > plane
        following = jnp.where(up, plane + 1, plane - 1)
        way = jnp.where(up, 0, 1)
        first = (which * 3 + way) * lane_sems

        @pl.when(following == target)
        def _():
            for d in range(inner):
                where = (place + d) % inner
                act_on(
                    remote(
                        term_send.at[which, target, where],
                        term_end.at[which, way, place],
                        term_sems,
                        first + planes + d,
                        following * inner + where,
                        first + planes + place,
                    )
                )

        @pl.when(following != target)
        def _():
            act_on(
                remote(
                    term_send.at[which, target],
                    term_hop.at[which, target],
                    term_sems,
                    first + target,
                    following * inner + place,
                )
            )

    def start(copy):
        copy.start()

    def send_terms(which, rows):
        for i in range(planes):
            target = turn(i)
            lhs = act_t[pl.ds(pl.multiple_of(target * (inner * shard), 16), inner * shard), :]
            part = dot(lhs, rows, NT)
            term_send[which, target] = part.astype(BF16).reshape(inner, shard, 2 * span)

            @pl.when(ends & (target != plane) & (target != neighbour))
            def _():
                move_terms(which, target, start)

    def own_terms(which):
        first = (which * 3 + 2) * lane_sems + planes
        for d in range(1, inner):
            where = (place + d) % inner
            copy = remote(
                term_send.at[which, plane, where],
                term_end.at[which, 2, place],
                term_sems,
                first + d,
                near(where),
                first + place,
            )
            copy.start()
            sent.append(copy)
        term_end[which, 2, place] = term_send[which, plane, place]

    def relay_terms(which, i):
        target = turn(i)

        @pl.when(jnp.logical_not(ends) & (target != plane))
        def _():
            way = jnp.where(target > plane, 0, 1)
            slot = (which * 3 + way) * lane_sems + target
            remote(
                term_send.at[which, target], term_hop.at[which, target], term_sems, slot, near(across)
            ).wait_recv()
            held = term_send[which, target].astype(F32) + term_hop[which, target].astype(F32)
            term_send[which, target] = held.astype(BF16)
            move_terms(which, target, start)

    def settle_terms(which):
        for i in range(planes):
            target = turn(i)

            @pl.when(target != plane)
            def _():
                move_terms(which, target, lambda copy: copy.wait_send())

    def ended_terms(which, way):
        first = (which * 3 + way) * lane_sems + planes
        for q in range(inner):
            copy = remote(
                term_send.at[which, 0, 0], term_end.at[which, way, q], term_sems, 0, near(across), first + q
            )
            if way == 2:
                pl.when(place != q)(copy.wait_recv)
            else:
                copy.wait_recv()

    def late_terms(which):
        @pl.when(ends)
        def _():
            move_terms(which, neighbour, start)

    def move_wout(k, act_on):
        up = place > plane
        following = jnp.where(up, plane + 1, plane - 1)
        way = jnp.where(up, 0, 1)

        @pl.when((place != plane) & (following == place))
        def _():
            act_on(remote(wout_send.at[k], wout_end.at[way], wout_sems, 3 + k, following * inner + k, way))

        @pl.when((place != plane) & (following != place))
        def _():
            act_on(remote(wout_send.at[k], wout_hop.at[k], wout_sems, 3 + k, following * inner + place))

        @pl.when((place == plane) & (place != k))
        def _():
            act_on(remote(wout_send.at[k], wout_end.at[2], wout_sems, 3 + k, near(k), 2))

    def relay_wout(k):
        @pl.when(jnp.logical_not(wout_first))
        def _():
            remote(wout_send.at[k], wout_hop.at[k], wout_sems, 3 + k, near(across)).wait_recv()
            wout_send[k] = (wout_send[k].astype(F32) + wout_hop[k].astype(F32)).astype(BF16)
            move_wout(k, start)

    def side_by_side(rows):
        return jnp.concatenate([rows[:, s].reshape(2 * span, tokens) for s in range(inner)], axis=1)

    send_terms(0, side_by_side(rows_a))
    cot_across.wait_recv()
    cot_relay.wait_recv()
    cots = cot_all[...].reshape(total, feature)
    wout_send[...] = dot(gated_s[...].reshape(span, total), cots, NN).astype(BF16).reshape(wout_send.shape)

    @pl.when(place == plane)
    def _():
        wout_end[2] = wout_send[place]

    wout_first = ends | (place == plane)


    def backward(k, carry):
        summed = jnp.zeros((tokens, tokens), F32)
        for s in range(inner):
            at = slice(s * tokens, (s + 1) * tokens)
            query, keys, values = q_s[k, :, at], k_s[k, :, at], v_s[k, :, at]
            probs = probs_s[k, s]
            grad_probs = dot(values, ga_s[k, :, at], TN)
            grad_scores = probs * (grad_probs - jnp.sum(probs * grad_probs, axis=0, keepdims=True))
            scores_b = grad_scores.astype(BF16)
            rows_b[0, s, k] = (dot(keys, scores_b, NN) * scale).astype(BF16)
            rows_b[1, s, k] = (dot(query, scores_b, NT) * scale).astype(BF16)
            summed = summed + grad_scores
        score_send[:, k] = summed.reshape(tok, cols, tokens).astype(BF16)
        return carry

    lax.fori_loop(0, group_heads, backward, 0)

    scores = []
    for step in range(1, tok):
        peer = (me + step) % tok
        copy = remote(score_send.at[peer], score_recv.at[me], score_sems, step - 1, peer)
        copy.start()
        scores.append(copy)
    sent += scores
    score_recv[me] = score_send[me]
    relay_terms(0, 0)
    relay_terms(0, 1)
    rows = side_by_side(rows_b)
    send_terms(1, rows)

    @pl.when(wout_first)
    def _():
        for k in range(group_heads):
            move_wout(k, start)

    for i in range(2, planes):
        relay_terms(0, i)
    query_part = dot(jnp.ones((8, total), BF16), rows[:window], NT)

    for copy in scores:
        copy.wait_recv()
    for q in range(inner):
        for k in range(group_heads):
            part = score_recv[q, k].astype(F32)
            for i in range(1, planes):
                part = part + score_recv[i * inner + q, k].astype(F32)
            h = q * group_heads + k
            score_f[pl.ds(h * cols, cols), :] = part
    weight_part = jnp.zeros((HEADS, channels), F32)
    gain_part = jnp.zeros((8, channels), F32)
    for j in range(cols):
        grad_bias = score_f[pl.ds(j, HEADS, stride=cols), :]
        y = normed[pl.ds(j, tokens, stride=cols), :]
        weight_part = weight_part + dot(grad_bias, y * gains, NN, lax.Precision.HIGHEST)
        grad_zg = dot(grad_bias, bias_w[...], TN, lax.Precision.HIGHEST)
        gain_part = gain_part + jnp.sum((y * grad_zg).reshape(tokens // 8, 8, channels), axis=0)
        g = grad_zg * gains
        first = jnp.mean(g, axis=-1, keepdims=True)
        second = jnp.mean(g * y, axis=-1, keepdims=True)
        pair_f[pl.ds(j, tokens, stride=cols), :] = (g - first - y * second) * rstd[pl.ds(j, tokens, stride=cols), :]
    grad_pair[...] = pair_f[...].reshape(tokens, cols, channels).astype(BF16)
    small_a[0:HEADS, :] = weight_part
    small_a[HEADS : HEADS + 8, :] = gain_part
    small_a[HEADS + 8 : HEADS + 16, :] = query_part[:, :128]
    small_a[HEADS + 16 : HEADS + 24, :] = query_part[:, 128:]
    firsts = []
    for d in range(1, inner):
        where = (place + d) % inner
        copy = remote(small_a, recv_a.at[place], small_sems, d, near(where))
        copy.start()
        firsts.append(copy)
    sent += firsts
    relay_terms(1, 0)
    relay_terms(1, 1)
    recv_a[place] = small_a[...]
    for copy in firsts:
        copy.wait_recv()
    held = recv_a[0, 0 : HEADS + 8, :]
    for q in range(1, inner):
        held = held + recv_a[q, 0 : HEADS + 8, :]
    small_b[0 : HEADS + 8, :] = held
    for q in range(inner):
        for half in range(2):
            at = HEADS + 8 + 8 * half
            small_b[HEADS + 8 + 2 * q + half : HEADS + 9 + 2 * q + half, :] = recv_a[q, at : at + 1, :]
    seconds = []
    for o in range(1, planes):
        target = (plane + o) % planes
        copy = remote(small_b, recv_b.at[plane], small_sems, inner + o, target * inner + place)
        copy.start()
        seconds.append(copy)
    sent += seconds
    recv_b[plane] = small_b[...]

    late_terms(0)
    late_terms(1)
    own_terms(0)
    own_terms(1)
    weights = jnp.concatenate([proj_t[b, pl.ds(offset, span), :] for b in range(4)], axis=0)

    def back_of(first, second):
        columns = []
        for s in (first, second):
            both = [x[:, s].reshape(2 * span, tokens) for x in (rows_b, rows_a)]
            columns.append(jnp.concatenate(both, axis=0))
        return dot(jnp.concatenate(columns, axis=1), weights, TN)

    back_send[0:2] = back_of(diagonal, across).astype(BF16).reshape(2, tokens, feature)
    backs = [remote(back_send.at[i], back_recv.at[i], back_sems, i, near(across)) for i in range(2)]
    for copy in backs:
        copy.start()
    back_part[...] = back_of(beside, place).reshape(2, tokens, feature)
    backs[0].wait_recv()
    back_send[2] = (back_part[0] + back_recv[0].astype(F32)).astype(BF16)
    backs.append(remote(back_send.at[2], back_recv.at[2], back_sems, 2, near(beside)))
    backs[2].start()
    sent += backs
    for i in range(2, planes):
        relay_terms(1, i)
    for k in range(group_heads):
        relay_wout(k)
    for copy in seconds:
        copy.wait_recv()
    held = recv_b[0]
    for i in range(1, planes):
        held = held + recv_b[i]
    small_out[...] = held[0:HEADS]
    gain_out[...] = jnp.sum(held[HEADS : HEADS + 8], axis=0)
    pieces = []
    for q in range(inner):
        at = HEADS + 8 + 2 * q
        pieces.append(jnp.concatenate([held[at : at + 1], held[at + 1 : at + 2, : span - 128]], axis=1))
    query_out[...] = jnp.concatenate(pieces, axis=1).reshape(feature)

    for copy in backs[1:]:
        copy.wait_recv()
    held = back_part[1] + back_recv[1].astype(F32) + back_recv[2].astype(F32)
    grad_act[...] = held.astype(BF16)

    def ended_wout(way):
        remote(wout_send.at[0], wout_end.at[way], wout_sems, 0, near(across), way).wait_recv()

    pl.when(plane > 0)(lambda: ended_wout(0))
    pl.when(plane < planes - 1)(lambda: ended_wout(1))
    pl.when(place != plane)(lambda: ended_wout(2))
    grad_out[...] = wout_end[2].astype(F32)

    @pl.when(plane > 0)
    def _():
        grad_out[...] += wout_end[0].astype(F32)

    @pl.when(plane < planes - 1)
    def _():
        grad_out[...] += wout_end[1].astype(F32)

    for which in range(2):
        ended_terms(which, 2)
        pl.when(plane > 0)(lambda: ended_terms(which, 0))
        pl.when(plane < planes - 1)(lambda: ended_terms(which, 1))
        sums = []
        for q in range(inner):
            held = term_end[which, 2, q].astype(F32)
            for there, way in ((plane > 0, 0), (plane < planes - 1, 1)):
                held = held + jnp.where(there, term_end[which, way, q].astype(F32), 0.0)
            sums.append(held)
        for b in range(2):
            at = (2 - 2 * which + b) * feature
            joined = jnp.concatenate([x[:, b * span : (b + 1) * span] for x in sums], axis=1)
            grad_w[:, at : at + feature] = joined
    for copy in sent:
        copy.wait_send()
    for k in range(group_heads):
        move_wout(k, lambda copy: copy.wait_send())
    for which in range(2):
        settle_terms(which)


def finish_kernel(*refs):
    count = len(refs) // 2
    ins, outs, sem = refs[:count], refs[count : 2 * count], refs[2 * count]
    copies = [pltpu.make_async_copy(ins[i], outs[i], sem.at[i]) for i in range(count)]
    for copy in copies:
        copy.start()
    for copy in copies:
        copy.wait()


def fused_plan(activations, pair_repr, pair_gain, bias_weight, proj_weight, query_bias, out_weight, token_mask, out_cotangent):
    samples, tokens, feature = activations.shape
    tok = lax.axis_size("tok")
    cols, channels = pair_repr.shape[1:]
    group_heads = HEADS // INNER
    planes = tok // INNER
    span = group_heads * HD
    window = -(-span // 128) * 128
    shard = feature // tok
    total = INNER * tokens
    small_rows = HEADS + 16

    def vmem(*shape, dtype=BF16):
        return pltpu.VMEM(shape, dtype)

    def sems(*shape):
        return pltpu.SemaphoreType.DMA(shape)

    scratch = [
        vmem(4, feature, window),
        vmem(feature, feature),
        vmem(tokens, cols, channels),
        vmem(channels, dtype=F32),
        vmem(feature, dtype=F32),
        vmem(tokens, dtype=jnp.int32),
        vmem(4, window, feature),
        vmem(INNER, tokens, feature),
        vmem(INNER, tokens, feature),
        vmem(feature, total),
        vmem(feature, 128, dtype=F32),
        vmem(tokens * cols, channels, dtype=F32),
        vmem(tokens * cols, channels, dtype=F32),
        vmem(cols * HEADS, tokens, dtype=F32),
        vmem(INNER, group_heads, cols, tokens),
        vmem(tok, group_heads, cols, tokens),
    ]
    scratch += [vmem(group_heads, HD, total)] * 7
    scratch += [
        vmem(INNER, group_heads, HD, tokens),
        vmem(INNER, group_heads, HD, tokens),
        vmem(group_heads, INNER, tokens, tokens, dtype=F32),
        vmem(2, INNER, group_heads, HD, tokens),
        vmem(2, INNER, group_heads, HD, tokens),
        vmem(2, tokens, feature, dtype=F32),
        vmem(3, tokens, feature),
        vmem(3, tokens, feature),
        vmem(2, planes, INNER, shard, 2 * span),
        vmem(2, planes, INNER, shard, 2 * span),
        vmem(2, 3, INNER, shard, 2 * span),
        vmem(group_heads, HD, feature),
        vmem(group_heads, HD, feature),
        vmem(3, HD, feature),
        vmem(tok, group_heads, cols, tokens),
        vmem(tok, group_heads, cols, tokens),
        vmem(HEADS * cols, tokens, dtype=F32),
        vmem(tokens * cols, channels, dtype=F32),
        vmem(HEADS + 24, channels, dtype=F32),
        vmem(small_rows, channels, dtype=F32),
        vmem(INNER, HEADS + 24, channels, dtype=F32),
        vmem(planes, small_rows, channels, dtype=F32),
        sems(11),
        sems(2, 6),
        sems(2, INNER),
        sems(2, tok - 1),
        sems(2, 6 * (planes + INNER)),
        sems(2, 3 + group_heads),
        sems(2, 3),
        sems(2, tok - 1),
        sems(2, INNER + planes),
    ]
    in_vmem = pl.BlockSpec(memory_space=pltpu.VMEM)
    in_hbm = pl.BlockSpec(memory_space=pltpu.HBM)
    shapes = [
        jax.ShapeDtypeStruct((tokens, feature), BF16),
        jax.ShapeDtypeStruct((tokens, cols, channels), BF16),
        jax.ShapeDtypeStruct((shard, 4 * feature), F32),
        jax.ShapeDtypeStruct((shard, feature), F32),
        jax.ShapeDtypeStruct((feature,), F32),
        jax.ShapeDtypeStruct((HEADS, channels), F32),
        jax.ShapeDtypeStruct((channels,), F32),
    ]
    results = pl.pallas_call(
        functools.partial(fused_kernel, tok),
        out_shape=shapes,
        in_specs=[in_hbm] * 4 + [in_vmem] + [in_hbm] * 4,
        out_specs=[in_vmem] * len(shapes),
        scratch_shapes=scratch,
        compiler_params=pltpu.CompilerParams(
            collective_id=3, has_side_effects=True, vmem_limit_bytes=67043328
        ),
        name="fused",
    )(
        activations.reshape(tokens, feature),
        out_cotangent.reshape(tokens, feature),
        pair_repr,
        pair_gain,
        bias_weight.T,
        query_bias,
        token_mask,
        proj_weight,
        out_weight,
    )
    results = pl.pallas_call(
        finish_kernel,
        out_shape=shapes,
        in_specs=[in_vmem] * len(shapes),
        out_specs=[in_hbm] * len(shapes),
        scratch_shapes=[pltpu.SemaphoreType.DMA((len(shapes),))],
        name="finish",
    )(*results)
    grad_act, grad_pair, grad_w, grad_out, query_sums, weight_sums, gain_sums = results
    return (
        grad_act.reshape(samples, tokens, feature),
        grad_pair,
        grad_w,
        grad_out,
        query_sums,
        weight_sums.T,
        gain_sums,
    )


def on_device(*args):
    samples, tokens, feature = args[0].shape
    tok = lax.axis_size("tok")
    cols, channels = args[1].shape[1:]
    square = tok == INNER * INNER and HEADS == tok and feature == HEADS * HD
    tiles = tokens == 128 and channels == 128 and tok * cols == tokens and cols % 8 == 0
    if samples == 1 and square and tiles:
        return fused_plan(*args)
    return general_plan(*args)


def solution(mesh):
    in_specs = (
        P(("groups", "tok"), None, None),
        P("groups", "tok", None),
        P(),
        P(),
        P(),
        P(),
        P(),
        P("groups"),
        P(("groups", "tok"), None, None),
    )
    out_specs = (
        P(("groups", "tok"), None, None),
        P("groups", "tok", None),
        P(("groups", "tok"), None),
        P(("groups", "tok"), None),
        P("groups"),
        P("groups", None),
        P("groups"),
    )
    return jax.shard_map(on_device, mesh=mesh, in_specs=in_specs, out_specs=out_specs, check_vma=False)
```

```python
import functools

import jax
import jax.numpy as jnp
from jax import lax
from jax.experimental import pallas as pl
from jax.experimental.pallas import tpu as pltpu
from jax.sharding import PartitionSpec as P

HEADS = 16
HD = 48
EPSILON = 1e-05
MASK_PENALTY = 10000.0
F32 = jnp.float32
BF16 = jnp.bfloat16
INNER = 4


def exchange_kernel(kinds, tok, *refs):
    count = len(kinds)
    ins, outs = refs[:count], refs[count : 2 * count]
    sends, recvs, local_sem = refs[2 * count : 3 * count], refs[3 * count : 4 * count], refs[4 * count]
    me = lax.axis_index("tok")
    group = me // INNER
    place = me % INNER
    across = place + 1 - 2 * (place % 2)
    beside = place + 2 - 4 * (place // 2)
    barrier = pltpu.get_barrier_semaphore()
    for step in range(1, tok):
        pl.semaphore_signal(barrier, inc=1, device_id={"tok": (me + step) % tok})
    pl.semaphore_wait(barrier, tok - 1)

    def send(k, slot, src, dst, peer):
        copy = pltpu.make_async_remote_copy(
            src_ref=src,
            dst_ref=dst,
            send_sem=sends[k].at[slot],
            recv_sem=recvs[k].at[slot],
            device_id={"tok": peer},
        )
        copy.start()
        return copy

    pending, relays, local = [], [], []
    for k, kind in enumerate(kinds):
        x, out = ins[k], outs[k]
        if kind == "near":
            first = send(k, 0, x, out.at[place], group * INNER + beside)
            pending.append(send(k, 1, x, out.at[place], group * INNER + across))
            relays.append((k, first, out.at[beside]))
        elif kind in ("all", "each"):
            for step in range(1, tok):
                peer = (me + step) % tok
                pending.append(send(k, step - 1, x if kind == "all" else x.at[peer], out.at[me], peer))
        elif kind == "near_each":
            for step in range(1, INNER):
                other = (place + step) % INNER
                pending.append(send(k, step - 1, x.at[other], out.at[place], group * INNER + other))
        else:
            for step in range(1, tok // INNER):
                other = (group + step) % (tok // INNER)
                pending.append(send(k, step - 1, x.at[other], out.at[group], other * INNER + place))
    for k, kind in enumerate(kinds):
        mine = {"all": me, "each": me, "near": place, "near_each": place, "far_each": group}[kind]
        own = ins[k] if kind in ("all", "near") else ins[k].at[mine]
        copy = pltpu.make_async_copy(own, outs[k].at[mine], local_sem.at[k])
        copy.start()
        local.append(copy)
    for k, first, block in relays:
        first.wait()
        pending.append(send(k, 2, block, block, group * INNER + across))
    for copy in local + pending:
        copy.wait()


def exchange(arrays, kinds, tok, collective_id):
    sizes = {"all": tok, "each": tok, "near": INNER, "near_each": INNER, "far_each": tok // INNER}
    shapes = []
    for x, kind in zip(arrays, kinds):
        block = x.shape if kind in ("all", "near") else x.shape[1:]
        shapes.append(jax.ShapeDtypeStruct((sizes[kind],) + block, x.dtype))
    sems = [pltpu.SemaphoreType.DMA((max(3, sizes[kind] - 1),)) for kind in kinds]
    return pl.pallas_call(
        functools.partial(exchange_kernel, kinds, tok),
        out_shape=shapes,
        in_specs=[pl.BlockSpec(memory_space=pltpu.VMEM)] * len(kinds),
        out_specs=[pl.BlockSpec(memory_space=pltpu.VMEM)] * len(kinds),
        scratch_shapes=sems + sems + [pltpu.SemaphoreType.DMA((len(kinds),))],
        compiler_params=pltpu.CompilerParams(
            collective_id=collective_id, has_side_effects=True, vmem_limit_bytes=40 * 2**20
        ),
        name=f"exchange_{collective_id}",
    )(*arrays)


def attention(query, keys, values, gate, grad_gated, bias_t, key_bias):
    scale = HD ** (-0.5)
    scores = jnp.einsum("hdj,hdi->hji", keys, query, preferred_element_type=F32) * scale
    scores = scores + bias_t.transpose(1, 0, 2).astype(F32) + key_bias[None, :, None]
    peak = jnp.max(scores, axis=1, keepdims=True)
    expo = jnp.exp(scores - peak)
    probs = expo / jnp.sum(expo, axis=1, keepdims=True)
    probs_b = probs.astype(BF16)
    attended = jnp.einsum("hdj,hji->hdi", values, probs_b, preferred_element_type=F32).astype(BF16)
    gate32 = gate.astype(F32)
    grad32 = grad_gated.astype(F32)
    att32 = attended.astype(F32)
    gated = (gate32 * att32).astype(BF16)
    grad_att = (grad32 * gate32).astype(BF16)
    grad_logit = (grad32 * att32 * gate32 * (1.0 - gate32)).astype(BF16)
    grad_probs = jnp.einsum("hdj,hdi->hji", values, grad_att, preferred_element_type=F32)
    grad_scores = probs * (grad_probs - jnp.sum(probs * grad_probs, axis=1, keepdims=True))
    scores_b = grad_scores.astype(BF16)
    grad_query = (jnp.einsum("hdj,hji->hdi", keys, scores_b, preferred_element_type=F32) * scale).astype(BF16)
    grad_key = (jnp.einsum("hdi,hji->hdj", query, scores_b, preferred_element_type=F32) * scale).astype(BF16)
    grad_value = jnp.einsum("hdi,hji->hdj", grad_att, probs_b, preferred_element_type=F32).astype(BF16)
    return jnp.stack([grad_query, grad_key, grad_value, grad_logit]), gated, grad_scores


def general_plan(activations, pair_repr, pair_gain, bias_weight, proj_weight, query_bias, out_weight, token_mask, out_cotangent):
    samples, tokens, feature = activations.shape
    tok = lax.axis_size("tok")
    cols = pair_repr.shape[1]
    act = activations.reshape(samples * tokens, feature)
    cot = out_cotangent.reshape(samples * tokens, feature)
    pair_f = pair_repr.astype(F32)
    centred = pair_f - jnp.mean(pair_f, axis=-1, keepdims=True)
    rstd = lax.rsqrt(jnp.mean(centred * centred, axis=-1, keepdims=True) + EPSILON)
    normed = centred * rstd
    scaled = normed * pair_gain
    bias_cols = jnp.einsum("ijc,ch->jhi", scaled, bias_weight, precision=lax.Precision.HIGHEST).astype(BF16)
    outer = tok // INNER
    shard = feature // tok

    def near_blocks(x):
        blocks = x.reshape(outer, INNER, shard, samples * tokens).transpose(1, 0, 2, 3)
        return blocks.reshape(INNER, outer * shard, samples * tokens)

    bias_t, cot_near, act_near = exchange(
        (bias_cols, cot, near_blocks(act.T)), ("all", "near", "near_each"), tok, 0
    )
    bias_t = bias_t.reshape((tok * cols,) + bias_cols.shape[1:])
    proj = jnp.einsum("tf,fn->nt", act, proj_weight, preferred_element_type=F32)
    proj = proj.reshape(4, feature, samples * tokens)
    query = (proj[0] + query_bias[:, None]).astype(BF16)
    keys = proj[1].astype(BF16)
    values = proj[2].astype(BF16)
    gate = jax.nn.sigmoid(proj[3]).astype(BF16)
    grad_gated = jnp.einsum("tn,mn->mt", cot, out_weight, preferred_element_type=F32).astype(BF16)
    key_bias = (token_mask.astype(F32) - 1.0) * MASK_PENALTY

    def heads_of(x):
        return x.reshape(HEADS, HD, samples, tokens).transpose(2, 0, 1, 3)

    grads, gated, grad_scores = jax.vmap(attention, in_axes=(0, 0, 0, 0, 0, None, None))(
        heads_of(query), heads_of(keys), heads_of(values), heads_of(gate), heads_of(grad_gated), bias_t, key_bias
    )
    grad_rows = grads.transpose(1, 2, 3, 0, 4).reshape(4 * feature, samples * tokens)
    gated_t = gated.transpose(1, 2, 0, 3).reshape(feature, samples * tokens)
    score_sum = jnp.sum(grad_scores, axis=0).astype(BF16)
    outgoing = score_sum.reshape(HEADS, tok, cols, tokens).transpose(1, 2, 0, 3)
    received, rows_near, gated_near = exchange(
        (outgoing, grad_rows, near_blocks(gated_t)), ("each", "near", "near_each"), tok, 1
    )
    grad_bias = jnp.sum(received.astype(F32), axis=0)
    grad_activations = jnp.einsum("nt,fn->tf", grad_rows, proj_weight, preferred_element_type=F32).astype(BF16)
    grad_zg = jnp.einsum("jhi,ch->ijc", grad_bias, bias_weight, precision=lax.Precision.HIGHEST)
    weight_part = jnp.einsum("ijc,jhi->ch", scaled, grad_bias, precision=lax.Precision.HIGHEST)
    gain_part = jnp.sum(normed * grad_zg, axis=(0, 1))
    query_part = jnp.sum(grad_rows[:feature].astype(F32), axis=1)
    small = jnp.concatenate([query_part, weight_part.reshape(-1), gain_part])
    small = jnp.pad(small, (0, -small.size % 1024)).reshape(-1, 128)
    first = jnp.einsum("srt,snt->rn", act_near, rows_near, preferred_element_type=F32)
    second = jnp.einsum("srt,stn->rn", gated_near, cot_near, preferred_element_type=F32)
    terms = jnp.concatenate([first.astype(BF16), second.astype(BF16)], axis=1)
    terms, small = exchange((terms.reshape(outer, shard, -1), small), ("far_each", "all"), tok, 2)
    weight_grads = jnp.sum(terms.astype(F32), axis=0)
    small = jnp.sum(small, axis=0).reshape(-1)
    grad_norm = grad_zg * pair_gain
    grad_pair = (
        grad_norm
        - jnp.mean(grad_norm, axis=-1, keepdims=True)
        - normed * jnp.mean(grad_norm * normed, axis=-1, keepdims=True)
    ) * rstd
    split = feature + weight_part.size
    return (
        grad_activations.reshape(samples, tokens, feature),
        grad_pair.astype(BF16),
        weight_grads[:, : 4 * feature],
        weight_grads[:, 4 * feature :],
        small[:feature],
        small[feature:split].reshape(weight_part.shape),
        small[split : split + pair_gain.shape[0]],
    )


NN = (((1,), (0,)), ((), ()))
NT = (((1,), (1,)), ((), ()))
TN = (((0,), (0,)), ((), ()))


def dot(a, b, dims, precision=None):
    return lax.dot_general(a, b, dims, precision=precision, preferred_element_type=F32)


def fused_kernel(
    tok,
    act,
    cot,
    pair_hbm,
    gain_hbm,
    bias_w,
    query_hbm,
    mask_hbm,
    proj_hbm,
    out_w_hbm,
    grad_act,
    grad_pair,
    grad_w,
    grad_out,
    query_out,
    small_out,
    gain_out,
    proj_w,
    out_w,
    pair,
    gain,
    query_bias,
    mask,
    proj_t,
    act_all,
    cot_all,
    act_t,
    query_col,
    normed,
    rstd,
    bias_f,
    bias_send,
    bias_recv,
    q_s,
    k_s,
    v_s,
    g_s,
    att_s,
    ga_s,
    gated_s,
    gg_send,
    gg_s,
    probs_s,
    rows_a,
    rows_b,
    back_part,
    back_send,
    back_recv,
    term_send,
    term_hop,
    term_end,
    wout_send,
    wout_hop,
    wout_end,
    score_send,
    score_recv,
    score_f,
    pair_f,
    small_a,
    small_b,
    recv_a,
    recv_b,
    local_sem,
    act_sems,
    gg_sems,
    bias_sems,
    term_sems,
    wout_sems,
    back_sems,
    score_sems,
    small_sems,
):
    tokens, feature = act.shape
    inner = INNER
    planes = tok // inner
    group_heads, head_dim = q_s.shape[0], q_s.shape[1]
    cols = pair.shape[1]
    channels = pair.shape[2]
    span = group_heads * head_dim
    window = proj_t.shape[1]
    shard = feature // tok
    scale = head_dim ** (-0.5)
    me = lax.axis_index("tok")
    plane = me // inner
    place = me % inner
    across = place + 1 - 2 * (place % 2)
    beside = place + 2 - 4 * (place // 2)
    diagonal = across + 2 - 4 * (across // 2)
    base = pl.multiple_of((place * span) // 128 * 128, 128)
    offset = pl.multiple_of(place * span - (place * span) // 128 * 128, 64)

    def load(src, dst, slot):
        copy = pltpu.make_async_copy(src, dst, local_sem.at[slot])
        copy.start()
        return copy

    load_act = load(act, act_all.at[place], 0)
    load_pair = load(pair_hbm, pair, 1)
    load_cot = load(cot, cot_all.at[place], 2)
    load_small = [load(gain_hbm, gain, 3), load(query_hbm, query_bias, 4), load(mask_hbm, mask, 5)]
    load_out = load(out_w_hbm, out_w, 6)
    load_proj = [
        load(proj_hbm.at[:, pl.ds(pl.multiple_of(feature * b + base, 128), window)], proj_w.at[b], 7 + b)
        for b in range(4)
    ]

    barrier = pltpu.get_barrier_semaphore()
    for step in range(1, tok):
        pl.semaphore_signal(barrier, inc=1, device_id={"tok": (me + step) % tok})

    def remote(src, dst, sems, slot, peer, arrival=None):
        return pltpu.make_async_remote_copy(
            src_ref=src,
            dst_ref=dst,
            send_sem=sems.at[0, slot],
            recv_sem=sems.at[1, slot if arrival is None else arrival],
            device_id={"tok": peer},
        )

    def near(where):
        return plane * inner + where

    sent = []
    load_pair.wait()
    for copy in load_small:
        copy.wait()
    gains = gain[...].reshape(1, channels)
    x = pair[...].astype(F32).reshape(tokens * cols, channels)
    centred = x - jnp.mean(x, axis=-1, keepdims=True)
    r = lax.rsqrt(jnp.mean(centred * centred, axis=-1, keepdims=True) + EPSILON)
    normed[...] = centred * r
    rstd[...] = jnp.broadcast_to(r, (tokens * cols, channels))
    for j in range(cols):
        y = normed[pl.ds(j, tokens, stride=cols), :]
        part = dot(bias_w[...], y * gains, NT, lax.Precision.HIGHEST)
        bias_f[pl.ds(j * HEADS, HEADS), :] = part
    for h in range(HEADS):
        bias_send[h // group_heads, h % group_heads] = bias_f[pl.ds(h, cols, stride=HEADS), :].astype(BF16)
    load_act.wait()
    pl.semaphore_wait(barrier, tok - 1)
    mine = act_all.at[place]
    act_beside = remote(mine, mine, act_sems, 0, near(beside))
    act_across = remote(mine, mine, act_sems, 1, near(across))
    for copy in (act_beside, act_across):
        copy.start()
        sent.append(copy)
    bias_copies = []
    for step in range(1, tok):
        peer = (me + step) % tok
        copy = remote(bias_send.at[peer % inner], bias_recv.at[me], bias_sems, step - 1, peer)
        copy.start()
        bias_copies.append(copy)
    sent += bias_copies
    load_cot.wait()
    load_out.wait()
    parts = dot(out_w[...], cot_all[place], NT).astype(BF16)
    gg_send[...] = parts.reshape(gg_send.shape)
    gg_copies = []
    for d in range(1, inner):
        where = (place + d) % inner
        copy = remote(gg_send.at[where], gg_s.at[place], gg_sems, d, near(where))
        copy.start()
        gg_copies.append(copy)
    sent += gg_copies
    mine = cot_all.at[place]
    cot_beside = remote(mine, mine, act_sems, 2, near(beside))
    cot_across = remote(mine, mine, act_sems, 3, near(across))
    for copy in (cot_beside, cot_across):
        copy.start()
        sent.append(copy)
    bias_recv[me] = bias_send[place]
    gg_s[place] = gg_send[place]

    shifts = query_bias[...].reshape(1, feature)
    row = jnp.broadcast_to(shifts, (128, feature))
    for c in range(feature // 128):
        query_col[c * 128 : (c + 1) * 128, :] = row[:, c * 128 : (c + 1) * 128].T
    for b in range(4):
        load_proj[b].wait()
        proj_t[b] = proj_w[b].T

    act_beside.wait_recv()
    act_relay = remote(act_all.at[beside], act_all.at[beside], act_sems, 4, near(across))
    act_relay.start()
    sent.append(act_relay)
    act_across.wait_recv()
    act_relay.wait_recv()
    total = inner * tokens
    acts = act_all[...].reshape(total, feature)
    stored = (group_heads, head_dim, total)
    for b, target in enumerate((q_s, k_s, v_s, g_s)):
        block = dot(proj_t[b, pl.ds(offset, span), :], acts, NT)
        if b == 0:
            shift = query_col[pl.ds(pl.multiple_of(place * span, 64), span), :]
            block = block + jnp.concatenate([shift] * (total // 128), axis=1)
        if b == 3:
            block = jax.nn.sigmoid(block)
        target[...] = block.astype(BF16).reshape(stored)
    for copy in bias_copies:
        copy.wait_recv()

    key_row = jnp.broadcast_to((mask[...].reshape(1, tokens).astype(F32) - 1.0) * MASK_PENALTY, (tokens, tokens))
    key_bias = key_row.T

    def forward(k, carry):
        bias = bias_recv[:, k].astype(F32).reshape(tokens, tokens)
        for s in range(inner):
            at = slice(s * tokens, (s + 1) * tokens)
            query, keys, values = q_s[k, :, at], k_s[k, :, at], v_s[k, :, at]
            scores = dot(keys, query, TN) * scale + bias + key_bias
            expo = jnp.exp(scores - jnp.max(scores, axis=0, keepdims=True))
            probs = expo / jnp.sum(expo, axis=0, keepdims=True)
            probs_s[k, s] = probs
            attended = dot(values, probs.astype(BF16), NN).astype(BF16)
            att_s[k, :, at] = attended
            gated_s[k, :, at] = (g_s[k, :, at].astype(F32) * attended.astype(F32)).astype(BF16)
        return carry

    lax.fori_loop(0, group_heads, forward, 0)
    for i in range(inner):
        act_t[:, i * tokens : (i + 1) * tokens] = act_all[i].T
    for copy in gg_copies:
        copy.wait_recv()

    def gates(k, carry):
        for s in range(inner):
            at = slice(s * tokens, (s + 1) * tokens)
            gate32 = g_s[k, :, at].astype(F32)
            grad32 = gg_s[s, k].astype(F32)
            attended = att_s[k, :, at].astype(F32)
            grad_att = (grad32 * gate32).astype(BF16)
            ga_s[k, :, at] = grad_att
            rows_a[1, s, k] = (grad32 * attended * gate32 * (1.0 - gate32)).astype(BF16)
            rows_a[0, s, k] = dot(grad_att, probs_s[k, s].astype(BF16), NT).astype(BF16)
        return carry

    lax.fori_loop(0, group_heads, gates, 0)
    cot_beside.wait_recv()
    cot_relay = remote(cot_all.at[beside], cot_all.at[beside], act_sems, 5, near(across))
    cot_relay.start()
    sent.append(cot_relay)

    lane_sems = planes + inner
    ends = (plane == 0) | (plane == planes - 1)
    neighbour = jnp.where(plane < planes // 2, plane + 1, plane - 1)

    def turn(i):
        return jnp.where(plane < planes // 2, planes - 1 - i, i)

    def move_terms(which, target, act_on):
        up = target > plane
        following = jnp.where(up, plane + 1, plane - 1)
        way = jnp.where(up, 0, 1)
        first = (which * 3 + way) * lane_sems

        @pl.when(following == target)
        def _():
            for d in range(inner):
                where = (place + d) % inner
                act_on(
                    remote(
                        term_send.at[which, target, where],
                        term_end.at[which, way, place],
                        term_sems,
                        first + planes + d,
                        following * inner + where,
                        first + planes + place,
                    )
                )

        @pl.when(following != target)
        def _():
            act_on(
                remote(
                    term_send.at[which, target],
                    term_hop.at[which, target],
                    term_sems,
                    first + target,
                    following * inner + place,
                )
            )

    def start(copy):
        copy.start()

    def send_terms(which, rows):
        for i in range(planes):
            target = turn(i)
            lhs = act_t[pl.ds(pl.multiple_of(target * (inner * shard), 16), inner * shard), :]
            part = dot(lhs, rows, NT)
            term_send[which, target] = part.astype(BF16).reshape(inner, shard, 2 * span)

            @pl.when(ends & (target != plane) & (target != neighbour))
            def _():
                move_terms(which, target, start)

    def own_terms(which):
        first = (which * 3 + 2) * lane_sems + planes
        for d in range(1, inner):
            where = (place + d) % inner
            copy = remote(
                term_send.at[which, plane, where],
                term_end.at[which, 2, place],
                term_sems,
                first + d,
                near(where),
                first + place,
            )
            copy.start()
            sent.append(copy)
        term_end[which, 2, place] = term_send[which, plane, place]

    def relay_terms(which, i):
        target = turn(i)

        @pl.when(jnp.logical_not(ends) & (target != plane))
        def _():
            way = jnp.where(target > plane, 0, 1)
            slot = (which * 3 + way) * lane_sems + target
            remote(
                term_send.at[which, target], term_hop.at[which, target], term_sems, slot, near(across)
            ).wait_recv()
            held = term_send[which, target].astype(F32) + term_hop[which, target].astype(F32)
            term_send[which, target] = held.astype(BF16)
            move_terms(which, target, start)

    def settle_terms(which):
        for i in range(planes):
            target = turn(i)

            @pl.when(target != plane)
            def _():
                move_terms(which, target, lambda copy: copy.wait_send())

    def ended_terms(which, way):
        first = (which * 3 + way) * lane_sems + planes
        for q in range(inner):
            copy = remote(
                term_send.at[which, 0, 0], term_end.at[which, way, q], term_sems, 0, near(across), first + q
            )
            if way == 2:
                pl.when(place != q)(copy.wait_recv)
            else:
                copy.wait_recv()

    def late_terms(which):
        @pl.when(ends)
        def _():
            move_terms(which, neighbour, start)

    def move_wout(k, act_on):
        up = place > plane
        following = jnp.where(up, plane + 1, plane - 1)
        way = jnp.where(up, 0, 1)

        @pl.when((place != plane) & (following == place))
        def _():
            act_on(remote(wout_send.at[k], wout_end.at[way], wout_sems, 3 + k, following * inner + k, way))

        @pl.when((place != plane) & (following != place))
        def _():
            act_on(remote(wout_send.at[k], wout_hop.at[k], wout_sems, 3 + k, following * inner + place))

        @pl.when((place == plane) & (place != k))
        def _():
            act_on(remote(wout_send.at[k], wout_end.at[2], wout_sems, 3 + k, near(k), 2))

    def relay_wout(k):
        @pl.when(jnp.logical_not(wout_first))
        def _():
            remote(wout_send.at[k], wout_hop.at[k], wout_sems, 3 + k, near(across)).wait_recv()
            wout_send[k] = (wout_send[k].astype(F32) + wout_hop[k].astype(F32)).astype(BF16)
            move_wout(k, start)

    def side_by_side(rows):
        return jnp.concatenate([rows[:, s].reshape(2 * span, tokens) for s in range(inner)], axis=1)

    send_terms(0, side_by_side(rows_a))
    cot_across.wait_recv()
    cot_relay.wait_recv()
    cots = cot_all[...].reshape(total, feature)
    wout_send[...] = dot(gated_s[...].reshape(span, total), cots, NN).astype(BF16).reshape(wout_send.shape)

    @pl.when(place == plane)
    def _():
        wout_end[2] = wout_send[place]

    wout_first = ends | (place == plane)


    def backward(k, carry):
        summed = jnp.zeros((tokens, tokens), F32)
        for s in range(inner):
            at = slice(s * tokens, (s + 1) * tokens)
            query, keys, values = q_s[k, :, at], k_s[k, :, at], v_s[k, :, at]
            probs = probs_s[k, s]
            grad_probs = dot(values, ga_s[k, :, at], TN)
            grad_scores = probs * (grad_probs - jnp.sum(probs * grad_probs, axis=0, keepdims=True))
            scores_b = grad_scores.astype(BF16)
            rows_b[0, s, k] = (dot(keys, scores_b, NN) * scale).astype(BF16)
            rows_b[1, s, k] = (dot(query, scores_b, NT) * scale).astype(BF16)
            summed = summed + grad_scores
        score_send[:, k] = summed.reshape(tok, cols, tokens).astype(BF16)
        return carry

    lax.fori_loop(0, group_heads, backward, 0)

    scores = []
    for step in range(1, tok):
        peer = (me + step) % tok
        copy = remote(score_send.at[peer], score_recv.at[me], score_sems, step - 1, peer)
        copy.start()
        scores.append(copy)
    sent += scores
    score_recv[me] = score_send[me]
    relay_terms(0, 0)
    relay_terms(0, 1)
    rows = side_by_side(rows_b)
    send_terms(1, rows)

    @pl.when(wout_first)
    def _():
        for k in range(group_heads):
            move_wout(k, start)

    query_part = dot(jnp.ones((8, total), BF16), rows[:window], NT)

    for copy in scores:
        copy.wait_recv()
    for q in range(inner):
        for k in range(group_heads):
            part = score_recv[q, k].astype(F32)
            for i in range(1, planes):
                part = part + score_recv[i * inner + q, k].astype(F32)
            h = q * group_heads + k
            score_f[pl.ds(h * cols, cols), :] = part
    weight_part = jnp.zeros((HEADS, channels), F32)
    gain_part = jnp.zeros((8, channels), F32)
    for j in range(cols):
        grad_bias = score_f[pl.ds(j, HEADS, stride=cols), :]
        y = normed[pl.ds(j, tokens, stride=cols), :]
        weight_part = weight_part + dot(grad_bias, y * gains, NN, lax.Precision.HIGHEST)
        grad_zg = dot(grad_bias, bias_w[...], TN, lax.Precision.HIGHEST)
        gain_part = gain_part + jnp.sum((y * grad_zg).reshape(tokens // 8, 8, channels), axis=0)
        g = grad_zg * gains
        first = jnp.mean(g, axis=-1, keepdims=True)
        second = jnp.mean(g * y, axis=-1, keepdims=True)
        pair_f[pl.ds(j, tokens, stride=cols), :] = (g - first - y * second) * rstd[pl.ds(j, tokens, stride=cols), :]
    grad_pair[...] = pair_f[...].reshape(tokens, cols, channels).astype(BF16)
    small_a[0:HEADS, :] = weight_part
    small_a[HEADS : HEADS + 8, :] = gain_part
    small_a[HEADS + 8 : HEADS + 16, :] = query_part[:, :128]
    small_a[HEADS + 16 : HEADS + 24, :] = query_part[:, 128:]
    firsts = []
    for d in range(1, inner):
        where = (place + d) % inner
        copy = remote(small_a, recv_a.at[place], small_sems, d, near(where))
        copy.start()
        firsts.append(copy)
    sent += firsts
    for i in range(2, planes):
        relay_terms(0, i)
    relay_terms(1, 0)
    relay_terms(1, 1)
    recv_a[place] = small_a[...]
    for copy in firsts:
        copy.wait_recv()
    held = recv_a[0, 0 : HEADS + 8, :]
    for q in range(1, inner):
        held = held + recv_a[q, 0 : HEADS + 8, :]
    small_b[0 : HEADS + 8, :] = held
    for q in range(inner):
        for half in range(2):
            at = HEADS + 8 + 8 * half
            small_b[HEADS + 8 + 2 * q + half : HEADS + 9 + 2 * q + half, :] = recv_a[q, at : at + 1, :]
    seconds = []
    for o in range(1, planes):
        target = (plane + o) % planes
        copy = remote(small_b, recv_b.at[plane], small_sems, inner + o, target * inner + place)
        copy.start()
        seconds.append(copy)
    sent += seconds
    recv_b[plane] = small_b[...]

    late_terms(0)
    late_terms(1)
    own_terms(0)
    own_terms(1)
    weights = jnp.concatenate([proj_t[b, pl.ds(offset, span), :] for b in range(4)], axis=0)

    def back_of(first, second):
        columns = []
        for s in (first, second):
            both = [x[:, s].reshape(2 * span, tokens) for x in (rows_b, rows_a)]
            columns.append(jnp.concatenate(both, axis=0))
        return dot(jnp.concatenate(columns, axis=1), weights, TN)

    back_send[0:2] = back_of(diagonal, across).astype(BF16).reshape(2, tokens, feature)
    backs = [remote(back_send.at[i], back_recv.at[i], back_sems, i, near(across)) for i in range(2)]
    for copy in backs:
        copy.start()
    back_part[...] = back_of(beside, place).reshape(2, tokens, feature)
    backs[0].wait_recv()
    back_send[2] = (back_part[0] + back_recv[0].astype(F32)).astype(BF16)
    backs.append(remote(back_send.at[2], back_recv.at[2], back_sems, 2, near(beside)))
    backs[2].start()
    sent += backs
    for i in range(2, planes):
        relay_terms(1, i)
    for k in range(group_heads):
        relay_wout(k)
    for copy in seconds:
        copy.wait_recv()
    held = recv_b[0]
    for i in range(1, planes):
        held = held + recv_b[i]
    small_out[...] = held[0:HEADS]
    gain_out[...] = jnp.sum(held[HEADS : HEADS + 8], axis=0)
    pieces = []
    for q in range(inner):
        at = HEADS + 8 + 2 * q
        pieces.append(jnp.concatenate([held[at : at + 1], held[at + 1 : at + 2, : span - 128]], axis=1))
    query_out[...] = jnp.concatenate(pieces, axis=1).reshape(feature)

    for copy in backs[1:]:
        copy.wait_recv()
    held = back_part[1] + back_recv[1].astype(F32) + back_recv[2].astype(F32)
    grad_act[...] = held.astype(BF16)

    def ended_wout(way):
        remote(wout_send.at[0], wout_end.at[way], wout_sems, 0, near(across), way).wait_recv()

    pl.when(plane > 0)(lambda: ended_wout(0))
    pl.when(plane < planes - 1)(lambda: ended_wout(1))
    pl.when(place != plane)(lambda: ended_wout(2))
    grad_out[...] = wout_end[2].astype(F32)

    @pl.when(plane > 0)
    def _():
        grad_out[...] += wout_end[0].astype(F32)

    @pl.when(plane < planes - 1)
    def _():
        grad_out[...] += wout_end[1].astype(F32)

    for which in range(2):
        ended_terms(which, 2)
        pl.when(plane > 0)(lambda: ended_terms(which, 0))
        pl.when(plane < planes - 1)(lambda: ended_terms(which, 1))
        sums = []
        for q in range(inner):
            held = term_end[which, 2, q].astype(F32)
            for there, way in ((plane > 0, 0), (plane < planes - 1, 1)):
                held = held + jnp.where(there, term_end[which, way, q].astype(F32), 0.0)
            sums.append(held)
        for b in range(2):
            at = (2 - 2 * which + b) * feature
            joined = jnp.concatenate([x[:, b * span : (b + 1) * span] for x in sums], axis=1)
            grad_w[:, at : at + feature] = joined
    for copy in sent:
        copy.wait_send()
    for k in range(group_heads):
        move_wout(k, lambda copy: copy.wait_send())
    for which in range(2):
        settle_terms(which)


def finish_kernel(*refs):
    count = len(refs) // 2
    ins, outs, sem = refs[:count], refs[count : 2 * count], refs[2 * count]
    copies = [pltpu.make_async_copy(ins[i], outs[i], sem.at[i]) for i in range(count)]
    for copy in copies:
        copy.start()
    for copy in copies:
        copy.wait()


def fused_plan(activations, pair_repr, pair_gain, bias_weight, proj_weight, query_bias, out_weight, token_mask, out_cotangent):
    samples, tokens, feature = activations.shape
    tok = lax.axis_size("tok")
    cols, channels = pair_repr.shape[1:]
    group_heads = HEADS // INNER
    planes = tok // INNER
    span = group_heads * HD
    window = -(-span // 128) * 128
    shard = feature // tok
    total = INNER * tokens
    small_rows = HEADS + 16

    def vmem(*shape, dtype=BF16):
        return pltpu.VMEM(shape, dtype)

    def sems(*shape):
        return pltpu.SemaphoreType.DMA(shape)

    scratch = [
        vmem(4, feature, window),
        vmem(feature, feature),
        vmem(tokens, cols, channels),
        vmem(channels, dtype=F32),
        vmem(feature, dtype=F32),
        vmem(tokens, dtype=jnp.int32),
        vmem(4, window, feature),
        vmem(INNER, tokens, feature),
        vmem(INNER, tokens, feature),
        vmem(feature, total),
        vmem(feature, 128, dtype=F32),
        vmem(tokens * cols, channels, dtype=F32),
        vmem(tokens * cols, channels, dtype=F32),
        vmem(cols * HEADS, tokens, dtype=F32),
        vmem(INNER, group_heads, cols, tokens),
        vmem(tok, group_heads, cols, tokens),
    ]
    scratch += [vmem(group_heads, HD, total)] * 7
    scratch += [
        vmem(INNER, group_heads, HD, tokens),
        vmem(INNER, group_heads, HD, tokens),
        vmem(group_heads, INNER, tokens, tokens, dtype=F32),
        vmem(2, INNER, group_heads, HD, tokens),
        vmem(2, INNER, group_heads, HD, tokens),
        vmem(2, tokens, feature, dtype=F32),
        vmem(3, tokens, feature),
        vmem(3, tokens, feature),
        vmem(2, planes, INNER, shard, 2 * span),
        vmem(2, planes, INNER, shard, 2 * span),
        vmem(2, 3, INNER, shard, 2 * span),
        vmem(group_heads, HD, feature),
        vmem(group_heads, HD, feature),
        vmem(3, HD, feature),
        vmem(tok, group_heads, cols, tokens),
        vmem(tok, group_heads, cols, tokens),
        vmem(HEADS * cols, tokens, dtype=F32),
        vmem(tokens * cols, channels, dtype=F32),
        vmem(HEADS + 24, channels, dtype=F32),
        vmem(small_rows, channels, dtype=F32),
        vmem(INNER, HEADS + 24, channels, dtype=F32),
        vmem(planes, small_rows, channels, dtype=F32),
        sems(11),
        sems(2, 6),
        sems(2, INNER),
        sems(2, tok - 1),
        sems(2, 6 * (planes + INNER)),
        sems(2, 3 + group_heads),
        sems(2, 3),
        sems(2, tok - 1),
        sems(2, INNER + planes),
    ]
    in_vmem = pl.BlockSpec(memory_space=pltpu.VMEM)
    in_hbm = pl.BlockSpec(memory_space=pltpu.HBM)
    shapes = [
        jax.ShapeDtypeStruct((tokens, feature), BF16),
        jax.ShapeDtypeStruct((tokens, cols, channels), BF16),
        jax.ShapeDtypeStruct((shard, 4 * feature), F32),
        jax.ShapeDtypeStruct((shard, feature), F32),
        jax.ShapeDtypeStruct((feature,), F32),
        jax.ShapeDtypeStruct((HEADS, channels), F32),
        jax.ShapeDtypeStruct((channels,), F32),
    ]
    results = pl.pallas_call(
        functools.partial(fused_kernel, tok),
        out_shape=shapes,
        in_specs=[in_hbm] * 4 + [in_vmem] + [in_hbm] * 4,
        out_specs=[in_vmem] * len(shapes),
        scratch_shapes=scratch,
        compiler_params=pltpu.CompilerParams(
            collective_id=3, has_side_effects=True, vmem_limit_bytes=67043328
        ),
        name="fused",
    )(
        activations.reshape(tokens, feature),
        out_cotangent.reshape(tokens, feature),
        pair_repr,
        pair_gain,
        bias_weight.T,
        query_bias,
        token_mask,
        proj_weight,
        out_weight,
    )
    results = pl.pallas_call(
        finish_kernel,
        out_shape=shapes,
        in_specs=[in_vmem] * len(shapes),
        out_specs=[in_hbm] * len(shapes),
        scratch_shapes=[pltpu.SemaphoreType.DMA((len(shapes),))],
        name="finish",
    )(*results)
    grad_act, grad_pair, grad_w, grad_out, query_sums, weight_sums, gain_sums = results
    return (
        grad_act.reshape(samples, tokens, feature),
        grad_pair,
        grad_w,
        grad_out,
        query_sums,
        weight_sums.T,
        gain_sums,
    )


def on_device(*args):
    samples, tokens, feature = args[0].shape
    tok = lax.axis_size("tok")
    cols, channels = args[1].shape[1:]
    square = tok == INNER * INNER and HEADS == tok and feature == HEADS * HD
    tiles = tokens == 128 and channels == 128 and tok * cols == tokens and cols % 8 == 0
    if samples == 1 and square and tiles:
        return fused_plan(*args)
    return general_plan(*args)


def solution(mesh):
    in_specs = (
        P(("groups", "tok"), None, None),
        P("groups", "tok", None),
        P(),
        P(),
        P(),
        P(),
        P(),
        P("groups"),
        P(("groups", "tok"), None, None),
    )
    out_specs = (
        P(("groups", "tok"), None, None),
        P("groups", "tok", None),
        P(("groups", "tok"), None),
        P(("groups", "tok"), None),
        P("groups"),
        P("groups", None),
        P("groups"),
    )
    return jax.shard_map(on_device, mesh=mesh, in_specs=in_specs, out_specs=out_specs, check_vma=False)
```
